32 devices in a mesh: obs: 8 (over z, x), chan: 4 (over y, core).
Axes of the slice: x: 2, y: 2, z: 4, core: 2. Of those that a mesh axis runs over, the one named last changes fastest.
Arguments:
- departures: bfloat16 [8192, 16384], P('chan', 'obs'), may hold values from -8 to 8
- predictors: bfloat16 [10, 16384], P(None, 'obs'), may hold values from -3 to 3
- inv_band: bfloat16 [63, 8192], P(None, 'chan'), may hold values from -1 to 2.5
- band_id: int32 [8192], replicated, may hold values from 0 to 340, never falling along the last dimension, each value on 1 to 32 neighbouring positions
- line_counts: int32 [128], P('obs'), may hold values from 24 to 128
Outputs:
- gram: float32 [100, 8192], P(None, ('chan', 'obs'))
- rhs: float32 [10, 8192], P(None, ('chan', 'obs'))
The draws below stay inside these ranges and needn't reach their ends.
Inputs may be any that keep to these rules, and one draw needn't show every extreme that they name: `band_id`: band numbers never fall along the channels; a band spans 1 to 32 channels. `line_counts`: slots of a scan line at or beyond its count are empty.
All inputs are finite; a program needn't handle non-finite values.
Results may differ from the reference program's by a relative error of at most 0.00062.
Values may be sent and summed in bfloat16 or wider, within the bound.
A program may use at most 64 MiB of HBM per device.

```python
import math
import jax
import jax.numpy as jnp
import numpy as np
from jax import lax

P_SIZE = 10
C = 8192
MAXB = 32
LINE_SLOTS = 128
LINES = 128
NOBS = 16384


def draw_inv_band(key, part):
    first_key, second_key = jax.random.split(jax.random.fold_in(key, 17))
    coupling = jnp.clip(0.2 * jax.random.normal(first_key, (2 * MAXB - 1, C), jnp.float32), -1.0, 1.0)
    center = jnp.exp(jax.random.uniform(second_key, (C,), jnp.float32, jnp.log(0.5), jnp.log(2.0)))
    rows_at = jnp.arange(2 * MAXB - 1)[:, None]
    return jnp.where(rows_at == MAXB - 1, center[None, :], coupling).astype(jnp.bfloat16)


def observation_predictors(key):
    value_key = jax.random.fold_in(jax.random.fold_in(key, 101), 1)
    place = jnp.arange(NOBS, dtype=jnp.float32) / jnp.float32(NOBS)
    rising = 0.7 * jnp.exp(jnp.log(3.0) * place)
    level = rising
    values = jax.random.uniform(value_key, (P_SIZE, NOBS), jnp.float32, -1.0, 1.0)
    return values * level[None, :]


def draw_predictors(key, part):
    return observation_predictors(key).astype(jnp.bfloat16)


def draw_departures(key, part):
    pred = observation_predictors(key)
    coef_key, scale_key, noise_key = jax.random.split(jax.random.fold_in(key, 202), 3)
    scales = jnp.exp(jax.random.uniform(scale_key, (C,), jnp.float32, jnp.log(0.2), jnp.log(1.2)))
    coefs = 0.5 * jax.random.normal(coef_key, (C, P_SIZE), jnp.float32) * scales[:, None]
    block = 128
    coef_blocks = coefs.reshape(C // block, block, P_SIZE)

    def one_block(index):
        bias = jnp.dot(coef_blocks[index], pred, precision=lax.Precision.HIGHEST)
        block_key = jax.random.fold_in(noise_key, index)
        noise = 0.5 * jax.random.normal(block_key, (block, NOBS), jnp.float32)
        return jnp.clip(bias + noise, -8.0, 8.0).astype(jnp.bfloat16)
    blocks = lax.map(one_block, jnp.arange(C // block, dtype=jnp.int32))
    return blocks.reshape(C, NOBS)


def set_ends(result, stream_key, smallest, largest):
    shape = result.shape
    spot = [jax.random.randint(jax.random.fold_in(stream_key, axis), (), 0, shape[axis]) for axis in range(len(shape))]
    result = result.at[tuple(spot)].set(smallest)
    longest = shape.index(max(shape))
    spot[longest] = (spot[longest] + 1) % shape[longest]
    return result.at[tuple(spot)].set(largest)


def split_up(count, total, most, skew):
    weights = [(1 << 20) // math.isqrt(grade ** skew) + 1 for grade in range(2, count + 1)]
    surplus, holding = total - most - (count - 1), [1] * (count - 1)
    while surplus > 0:
        free = [i for i in range(count - 1) if holding[i] < most]
        mass, remaining = sum([weights[i] for i in free]), surplus
        for i in free:
            addition = min(most - holding[i], max(1, remaining * weights[i] // mass), surplus)
            holding[i] = holding[i] + addition
            surplus = surplus - addition
    return np.array([most] + holding)


def ragged(stream_key, number_of, total, most, skew):
    if number_of == 2:
        one = jax.random.randint(stream_key, (), max(1, total - most), min(most, total - 1) + 1)
        return jnp.stack([one, total - one])
    lengths = jnp.asarray(split_up(number_of, total, most, skew), jnp.int32)
    pairs = (number_of - 1) // 2
    source_of, receiver = lengths[1:1 + 2 * pairs:2], lengths[2:2 + 2 * pairs:2]
    room = jnp.minimum(source_of - 1, most - receiver)
    shifted = jax.random.randint(jax.random.fold_in(stream_key, 1), (pairs,), 0, 1 << 20) % (room + 1)
    lengths = lengths.at[1:1 + 2 * pairs:2].set(source_of - shifted).at[2:2 + 2 * pairs:2].set(receiver + shifted)
    return lengths[jax.random.permutation(jax.random.fold_in(stream_key, 2), number_of)]


def setup_inputs(seed: int = 0) -> dict:
    streams_of = jax.random.split(jax.random.key(seed), 6)
    departures = draw_departures(jax.random.fold_in(streams_of[5], 71), 0)
    predictors = draw_predictors(jax.random.fold_in(streams_of[5], 71), 0)
    inv_band = draw_inv_band(jax.random.fold_in(streams_of[5], 71), 0)
    band_id = jnp.searchsorted(jnp.cumsum(ragged(streams_of[3], C // 24, C, MAXB, 1)), jnp.arange(C), side="right").astype(jnp.int32)
    line_counts = set_ends(jax.random.randint(streams_of[4], (LINES,), 24, LINE_SLOTS + 1), jax.random.fold_in(streams_of[4], 1), 24, LINE_SLOTS).astype(jnp.int32)
    return {"departures": departures, "predictors": predictors, "inv_band": inv_band, "band_id": band_id, "line_counts": line_counts}


huber_edge = 1.0


def reference(departures, predictors, inv_band, band_id, line_counts):
    chans, nobs = departures.shape
    half = MAXB - 1
    tile = 128
    extent = tile + 2 * half
    slots = jnp.arange(nobs, dtype=jnp.int32)
    live = (slots % LINE_SLOTS < jnp.repeat(line_counts, LINE_SLOTS)).astype(jnp.float32)
    pred_wide = predictors.astype(jnp.float32).T
    pairs_t = (pred_wide[:, :, None] * pred_wide[:, None, :]).reshape(nobs, P_SIZE * P_SIZE).astype(jnp.bfloat16)
    pred_t = predictors.T

    def one_tile(index):
        first = index * tile
        start = jnp.clip(first - half, 0, chans - extent).astype(jnp.int32)
        rows_at = first + jnp.arange(tile, dtype=jnp.int32)
        cols_at = start + jnp.arange(extent, dtype=jnp.int32)
        offset = cols_at[None, :] - rows_at[:, None] + half
        keep = (offset >= 0) & (offset <= 2 * half) & (band_id[cols_at][None, :] == band_id[rows_at][:, None])
        values = inv_band[jnp.clip(offset, 0, 2 * half), rows_at[:, None]]
        matrix = jnp.where(keep, values, jnp.zeros_like(values))
        window = lax.dynamic_slice_in_dim(departures, start, extent, 0)
        weighted = jnp.dot(matrix, window, preferred_element_type=jnp.float32)
        ratio = live[None, :] * (huber_edge / jnp.maximum(jnp.abs(weighted), huber_edge))
        qc_weight = ratio.astype(jnp.bfloat16)
        scaled = (ratio * weighted).astype(jnp.bfloat16)
        gram_tile = jnp.dot(qc_weight, pairs_t, preferred_element_type=jnp.float32)
        rhs_tile = jnp.dot(scaled, pred_t, preferred_element_type=jnp.float32)
        return gram_tile, rhs_tile

    grams, rhss = lax.map(one_tile, jnp.arange(chans // tile, dtype=jnp.int32))
    gram = grams.reshape(chans, P_SIZE * P_SIZE).T / jnp.float32(nobs)
    rhs = rhss.reshape(chans, P_SIZE).T / jnp.float32(nobs)
    return gram, rhs
```

```python
import functools

import jax
import jax.numpy as jnp
import numpy as np
from jax import lax
from jax.experimental import pallas as pl
from jax.experimental.pallas import tpu as pltpu
from jax.sharding import PartitionSpec as P

huber_edge = 1.0
LANES = 128
HALO = 32
TILE = 128
WIDTH = 2 * TILE
OBS_TILE = 256
CODE = 32512.0
MESH = pl.DeviceIdType.MESH


def mirror_rows(count):
    rows = []
    for first in range(count):
        for second in range(count):
            low = min(first, second)
            high = max(first, second)
            rows.append(low * count - low * (low - 1) // 2 + high - low)
    return rows


def padded(count, unit):
    return -(-count // unit) * unit


def peer(axis, index):
    if axis == "obs":
        return (index, lax.axis_index("chan"))
    return (lax.axis_index("obs"), index)


def kernel(n_obs, n_chan, scatter, dep, pred, inv, ids, counts, *rest):
    if scatter:
        gram_out, rhs_out = rest[:2]
        rest = rest[2:]
    else:
        part_out = rest[0]
        rest = rest[1:]
    (
        window,
        pred_in,
        inv_in,
        ids_in,
        counts_in,
        wide,
        pairs_t,
        preds_t,
        flip,
        bands,
        turned_w,
        mine,
        x_code,
        z_code,
        landed_x,
        landed_z,
        total,
        small_sem,
        load_sem,
        halo_send,
        halo_recv,
        x_send,
        x_recv,
        z_send,
        z_recv,
    ) = rest
    own, obs_dev = dep.shape
    preds = pred.shape[0]
    offsets = inv.shape[0]
    half = offsets // 2
    upper = preds * (preds + 1) // 2
    pad = padded(upper, 8)
    tall = pairs_t.shape[0]
    flat = preds_t.shape[0]
    blocks = own // WIDTH
    levels = blocks // 2
    stages = obs_dev // (2 * OBS_TILE)
    lines = counts.shape[0]
    slots = obs_dev // lines
    me = lax.axis_index("obs")
    chan = lax.axis_index("chan")
    right = lax.rem(chan + 1, n_chan)
    left = lax.rem(chan + n_chan - 1, n_chan)
    if scatter:
        col = lax.rem(me, 2)
        lev = lax.div(me, 2)
        partner = me + 1 - 2 * col
    else:
        col = 1
        lev = levels - 1
        partner = me
    early = lev == 0

    def level_at(turn):
        turn = jnp.int32(turn)
        return jnp.where(turn == levels - 1, lev, jnp.where(turn >= lev, turn + 1, turn))

    def first_col(turn):
        later = 1 - col if scatter else 0
        return jnp.where(turn == 0, jnp.where(early, col, 1), later)

    def block_at(step):
        step = jnp.int32(step)
        turn = lax.div(step, 2)
        first = first_col(turn)
        return 2 * level_at(turn) + jnp.where(lax.rem(step, 2) == 0, first, 1 - first)

    def for_partner(step):
        return lax.rem(block_at(step), 2) != col

    barrier = pltpu.get_barrier_semaphore()
    for index in (left, right):
        pl.semaphore_signal(barrier, inc=1, device_id=peer("chan", index), device_id_type=MESH)
    greeted = 2
    if scatter:
        pl.semaphore_signal(barrier, inc=1, device_id=peer("obs", partner), device_id_type=MESH)
        for turn in range(levels - 1):
            index = 2 * level_at(turn) + col
            pl.semaphore_signal(barrier, inc=1, device_id=peer("obs", index), device_id_type=MESH)
        greeted += levels

    base = pl.multiple_of(chan * own, own)
    smalls = [
        pltpu.make_async_copy(pred, pred_in, small_sem.at[0]),
        pltpu.make_async_copy(counts, counts_in, small_sem.at[1]),
        pltpu.make_async_copy(inv, inv_in, small_sem.at[2]),
        pltpu.make_async_copy(
            ids.at[:, pl.ds(base, own)], ids_in.at[:, pl.ds(LANES, own)], small_sem.at[3]
        ),
        pltpu.make_async_copy(
            ids.at[:, pl.ds(pl.multiple_of(jnp.maximum(base - LANES, 0), LANES), LANES)],
            ids_in.at[:, pl.ds(0, LANES)],
            small_sem.at[4],
        ),
        pltpu.make_async_copy(
            ids.at[
                :, pl.ds(pl.multiple_of(jnp.minimum(base + own, own * n_chan - LANES), LANES), LANES)
            ],
            ids_in.at[:, pl.ds(LANES + own, LANES)],
            small_sem.at[5],
        ),
    ]
    for copy in smalls:
        copy.start()

    def load(place):
        chunk = lax.rem(jnp.where(early, 1, 0) + place, blocks)
        start = pl.multiple_of(chunk * WIDTH, WIDTH)
        return pltpu.make_async_copy(
            dep.at[pl.ds(start, WIDTH), :],
            window.at[pl.ds(start + HALO, WIDTH), :],
            load_sem.at[place],
        )

    for place in range(blocks):
        load(place).start()

    to_left = pltpu.make_async_remote_copy(
        src_ref=dep.at[pl.ds(0, HALO), :],
        dst_ref=window.at[pl.ds(own + HALO, HALO), :],
        send_sem=halo_send.at[0],
        recv_sem=halo_recv.at[0],
        device_id=peer("chan", left),
        device_id_type=MESH,
    )
    to_right = pltpu.make_async_remote_copy(
        src_ref=dep.at[pl.ds(own - HALO, HALO), :],
        dst_ref=window.at[pl.ds(0, HALO), :],
        send_sem=halo_send.at[1],
        recv_sem=halo_recv.at[1],
        device_id=peer("chan", right),
        device_id_type=MESH,
    )

    def meet():
        pl.semaphore_wait(barrier, greeted)
        to_left.start()
        to_right.start()

    pl.when(jnp.logical_not(early))(meet)

    window[own + 2 * HALO :, :] = jnp.zeros((window.shape[0] - own - 2 * HALO, obs_dev), window.dtype)
    flip[...] = jnp.zeros_like(flip)
    wide[...] = jnp.zeros_like(wide)

    smalls[0].wait()
    smalls[1].wait()
    values = pred_in[...].astype(jnp.float32)
    first_row = 0
    for first in range(preds):
        count = preds - first
        wide[first_row : first_row + count, :] = values[first:, :] * values[first : first + 1, :]
        first_row += count
    wide[tall : tall + preds, :] = values

    def mask_line(line, carry):
        at = pl.ds(pl.multiple_of(line * slots, slots), slots)
        slot = lax.broadcasted_iota(jnp.int32, (tall + flat, slots), 1)
        live = jnp.where(slot < counts_in[line], wide[:, at], 0.0).astype(jnp.bfloat16)
        pairs_t[:, at] = live[:tall, :]
        preds_t[:, at] = live[tall:, :]
        return carry

    lax.fori_loop(0, lines, mask_line, 0, unroll=4)

    for copy in smalls[2:]:
        copy.wait()

    @pl.when(chan == 0)
    def _():
        ids_in[:, 0:LANES] = jnp.full((1, LANES), -1, jnp.int32)

    @pl.when(chan == n_chan - 1)
    def _():
        ids_in[:, LANES + own :] = jnp.full((1, LANES), -1, jnp.int32)

    def build(block, side):
        for part in range(2):
            first = pl.multiple_of(block * WIDTH + part * TILE, TILE)
            near = ids_in[:, pl.ds(first, 3 * TILE)].astype(jnp.float32)
            flip[part, 0:offsets, :] = inv_in[:, pl.ds(first, TILE)].astype(jnp.float32)
            flip[part, 64:65, :] = near[:, TILE : 2 * TILE]
            turned = flip[part].T
            own_id = turned[:, 64:65]
            place = lax.broadcasted_iota(jnp.int32, turned.shape, 1)
            turned = jnp.where(place < offsets, turned, 0.0)
            skewed = pltpu.roll(
                jnp.concatenate([turned, jnp.zeros_like(turned)], axis=1),
                HALO - half,
                1,
                stride=1,
                stride_axis=0,
            )
            same = near[:, TILE - HALO : 3 * TILE - HALO] == own_id
            bands[side, part * TILE : (part + 1) * TILE, :] = jnp.where(same, skewed, 0.0).astype(
                jnp.bfloat16
            )

    def send_x(turn):
        return pltpu.make_async_remote_copy(
            src_ref=x_code.at[turn],
            dst_ref=landed_x.at[turn],
            send_sem=x_send.at[turn],
            recv_sem=x_recv.at[turn],
            device_id=peer("obs", partner),
            device_id_type=MESH,
        )

    def send_z(turn):
        return pltpu.make_async_remote_copy(
            src_ref=z_code.at[turn],
            dst_ref=landed_z.at[lev],
            send_sem=z_send.at[turn],
            recv_sem=z_recv.at[lev],
            device_id=peer("obs", 2 * level_at(turn) + col),
            device_id_type=MESH,
        )

    def from_z(turn):
        sender = level_at(turn)
        return pltpu.make_async_remote_copy(
            src_ref=z_code.at[0],
            dst_ref=landed_z.at[sender],
            send_sem=z_send.at[0],
            recv_sem=z_recv.at[sender],
            device_id=peer("obs", 2 * sender + col),
            device_id_type=MESH,
        )

    def encode(sums):
        gram = sums[:pad]
        rhs = sums[pad:]

        def grade(part):
            most = jnp.max(jnp.abs(part), axis=0, keepdims=True)
            return jnp.ceil(jnp.log2(jnp.maximum(most, 1e-30)))

        gram_grade = grade(gram)
        rhs_grade = grade(rhs)
        row = lax.broadcasted_iota(jnp.int32, rhs.shape, 0)
        gram = gram * (jnp.exp2(-gram_grade) * CODE)
        rhs = rhs * (jnp.exp2(-rhs_grade) * CODE)
        rhs = jnp.where(row == preds, gram_grade, rhs)
        rhs = jnp.where(row == preds + 1, rhs_grade, rhs)
        return jnp.round(jnp.concatenate([gram, rhs], axis=0)).astype(jnp.int32).astype(jnp.int16)

    def decode(code):
        values = code.astype(jnp.int32).astype(jnp.float32)
        gram_scale = jnp.exp2(values[pad + preds : pad + preds + 1]) * (1.0 / CODE)
        rhs_scale = jnp.exp2(values[pad + preds + 1 : pad + preds + 2]) * (1.0 / CODE)
        return jnp.concatenate([values[:pad] * gram_scale, values[pad:] * rhs_scale], axis=0)

    def pass_on(turn):
        send_x(turn).wait_recv()
        z_code[turn] = encode(mine[turn] + decode(landed_x[turn]))
        send_z(turn).start()

    def accumulated(*accs):
        narrow = [[accs[4 * mxu + 2 * side : 4 * mxu + 2 * side + 2] for side in range(2)] for mxu in range(2)]
        tall_acc = [accs[8 + 2 * mxu : 10 + 2 * mxu] for mxu in range(2)]
        flat_acc = [accs[12 + 2 * mxu : 14 + 2 * mxu] for mxu in range(2)]

        def weigh(block, band, stage):
            start = pl.multiple_of(block * WIDTH, WIDTH)
            for mxu in range(2):
                at = (2 * stage + mxu) * OBS_TILE
                for part in range(2):
                    first = pl.multiple_of(start + part * TILE, TILE)
                    pltpu.matmul_push_rhs(
                        window[pl.ds(first, 2 * TILE), at : at + OBS_TILE],
                        staging_register=part,
                        mxu_index=mxu,
                    )
                    pltpu.matmul_acc_lhs(
                        narrow[mxu][stage % 2][part],
                        bands[band, part * TILE : (part + 1) * TILE, :],
                        load_staged_rhs=part,
                    )

        def turn_over(stage):
            for mxu in range(2):
                for part in range(2):
                    weighted = pltpu.matmul_pop(narrow[mxu][stage % 2][part])
                    turned_w[stage % 2, mxu, :, part * TILE : (part + 1) * TILE] = weighted.astype(
                        jnp.bfloat16
                    ).T

        def gather(side, stage):
            edge = jnp.bfloat16(huber_edge)
            for mxu in range(2):
                at = (2 * stage + mxu) * OBS_TILE
                weighted = turned_w[stage % 2, mxu]
                qc_weight = edge / jnp.maximum(jnp.abs(weighted), edge)
                scaled = jnp.clip(weighted, -edge, edge)
                pltpu.matmul_push_rhs(qc_weight, staging_register=0, mxu_index=mxu)
                pltpu.matmul_acc_lhs(
                    tall_acc[mxu][side], pairs_t[:, at : at + OBS_TILE], load_staged_rhs=0
                )
                pltpu.matmul_push_rhs(scaled, staging_register=1, mxu_index=mxu)
                pltpu.matmul_acc_lhs(
                    flat_acc[mxu][side], preds_t[:, at : at + OBS_TILE], load_staged_rhs=1
                )

        def result(side):
            gram = pltpu.matmul_pop(tall_acc[0][side]) + pltpu.matmul_pop(tall_acc[1][side])
            rhs = pltpu.matmul_pop(flat_acc[0][side]) + pltpu.matmul_pop(flat_acc[1][side])
            return jnp.concatenate([gram[:pad], rhs], axis=0)

        def deliver(step, sums):
            if not scatter:
                start = pl.multiple_of(block_at(step) * WIDTH, WIDTH)
                part_out[:, pl.ds(start, WIDTH)] = sums
                return
            turn = lax.div(step, 2)
            theirs = for_partner(step)

            @pl.when(theirs)
            def _():
                x_code[turn] = encode(sums)
                send_x(turn).start()

            @pl.when(jnp.logical_not(theirs))
            def _():
                mine[turn] = sums

        for acc in accs:
            pltpu.matmul_pop(acc)
        for place in range(4):
            load(place).wait()
        build(block_at(0), 0)
        weigh(block_at(0), 0, 0)
        weigh(block_at(0), 0, 1)
        turn_over(0)

        def one_turn(turn, carry):
            for side in range(2):
                step = 2 * turn + side
                block = block_at(step)
                following = block_at(jnp.minimum(step + 1, blocks - 1))
                more = step + 1 < blocks
                middle = stages // 2
                build(following, 1 - side)
                for stage in range(stages):
                    if stage == middle:
                        sums = result(1 - side)
                        if side == 1:

                            @pl.when(turn == 0)
                            def _():
                                for place in range(4, blocks):
                                    load(place).wait()

                            deliver(step - 1, sums)
                        else:

                            @pl.when(jnp.logical_and(early, turn == 1))
                            def _():
                                meet()

                            @pl.when(turn > 0)
                            def _():
                                deliver(step - 1, sums)

                            if scatter:

                                @pl.when(turn > 1)
                                def _():
                                    pass_on(turn - 2)

                        @pl.when(jnp.logical_and(more, following == 0))
                        def _():
                            to_right.wait_recv()

                        @pl.when(jnp.logical_and(more, following == blocks - 1))
                        def _():
                            to_left.wait_recv()

                    ahead = stage + 2
                    if ahead < stages:
                        weigh(block, side, ahead)
                    else:
                        weigh(following, 1 - side, ahead - stages)
                    turn_over((stage + 1) % stages)
                    gather(side, stage)
            return carry

        lax.fori_loop(0, levels, one_turn, 0)
        for mxu in range(2):
            for part in range(2):
                for side in range(2):
                    pltpu.matmul_pop(narrow[mxu][side][part])
        deliver(blocks - 1, result(1))

    pl.run_scoped(accumulated, *acc_list(tall, flat))
    to_left.wait_send()
    to_right.wait_send()

    if scatter:
        pass_on(levels - 2)
        last = levels - 1
        send_x(last).wait_recv()
        sums = mine[last] + decode(landed_x[last])
        for turn in range(levels - 1):
            from_z(turn).wait_recv()
            sums = sums + decode(landed_z[level_at(turn)])
        total[...] = sums * (1.0 / float(obs_dev * n_obs))
        for row, source in enumerate(mirror_rows(preds)):
            gram_out[row : row + 1, :] = total[source : source + 1, :]
        rhs_out[...] = total[pad : pad + preds, :]
        for turn in range(levels):
            send_x(turn).wait_send()
        for turn in range(levels - 1):
            send_z(turn).wait_send()


def acc_list(tall, flat):
    specs = []
    for rows, copies in ((TILE, 4), (tall, 2), (flat, 2)):
        for mxu in range(2):
            specs += [pltpu.ACC(mxu)((rows, OBS_TILE), jnp.float32)] * copies
    return specs


def on_device(departures, predictors, inv_band, band_id, line_counts):
    own, obs_dev = departures.shape
    preds = predictors.shape[0]
    upper = preds * (preds + 1) // 2
    n_obs = lax.axis_size("obs")
    n_chan = lax.axis_size("chan")
    share = own // n_obs
    blocks = own // WIDTH
    scatter = share == WIDTH and n_obs % 2 == 0 and n_obs >= 8
    pad = padded(upper, 8)
    tall = padded(upper, 16)
    flat = padded(preds + 2, 16)
    rows = pad + flat
    if scatter:
        out_shape = (
            pltpu.VMEM((preds * preds, share), jnp.float32),
            pltpu.VMEM((preds, share), jnp.float32),
        )
    else:
        out_shape = (jax.ShapeDtypeStruct((rows, own), jnp.float32),)
    vmem = pl.BlockSpec(memory_space=pltpu.VMEM)
    hbm = pl.BlockSpec(memory_space=pltpu.HBM)
    levels = blocks // 2
    kept = (levels, rows, WIDTH) if scatter else (1, 8, LANES)
    dma = pltpu.SemaphoreType.DMA
    outs = pl.pallas_call(
        functools.partial(kernel, n_obs, n_chan, scatter),
        out_shape=out_shape,
        in_specs=[hbm] * 5,
        out_specs=tuple(vmem for _ in out_shape),
        scratch_shapes=[
            pltpu.VMEM((own + 4 * HALO, obs_dev), jnp.bfloat16),
            pltpu.VMEM(predictors.shape, jnp.bfloat16),
            pltpu.VMEM(inv_band.shape, jnp.bfloat16),
            pltpu.VMEM((1, own + 2 * LANES), jnp.int32),
            pltpu.SMEM(line_counts.shape, jnp.int32),
            pltpu.VMEM((tall + flat, obs_dev), jnp.float32),
            pltpu.VMEM((tall, obs_dev), jnp.bfloat16),
            pltpu.VMEM((flat, obs_dev), jnp.bfloat16),
            pltpu.VMEM((2, LANES, TILE), jnp.float32),
            pltpu.VMEM((2, WIDTH, 2 * TILE), jnp.bfloat16),
            pltpu.VMEM((2, 2, OBS_TILE, WIDTH), jnp.bfloat16),
            pltpu.VMEM(kept, jnp.float32),
            pltpu.VMEM(kept, jnp.int16),
            pltpu.VMEM(kept, jnp.int16),
            pltpu.VMEM(kept, jnp.int16),
            pltpu.VMEM(kept, jnp.int16),
            pltpu.VMEM((rows, WIDTH), jnp.float32),
            dma((6,)),
            dma((blocks,)),
            dma((2,)),
            dma((2,)),
            dma((levels,)),
            dma((levels,)),
            dma((levels,)),
            dma((levels,)),
        ],
        compiler_params=pltpu.CompilerParams(
            collective_id=0,
            has_side_effects=True,
            vmem_limit_bytes=67043328 - 120 * 1024,
        ),
        name="normal_equations",
    )(departures, predictors, inv_band, band_id[None, :], line_counts)
    if scatter:
        return outs[0], outs[1]
    factor = 1.0 / float(obs_dev * n_obs)
    part = lax.psum_scatter(outs[0], "obs", scatter_dimension=1, tiled=True) * factor
    mirror = np.array(mirror_rows(preds))
    return part[mirror], part[pad : pad + preds]


def solution(mesh):
    in_specs = (P("chan", "obs"), P(None, "obs"), P(None, "chan"), P(), P("obs"))
    out_specs = (P(None, ("chan", "obs")), P(None, ("chan", "obs")))
    return jax.shard_map(
        on_device, mesh=mesh, in_specs=in_specs, out_specs=out_specs, check_vma=False
    )
```

```python
import functools

import jax
import jax.numpy as jnp
import numpy as np
from jax import lax
from jax.experimental import pallas as pl
from jax.experimental.pallas import tpu as pltpu
from jax.sharding import PartitionSpec as P

huber_edge = 1.0
LANES = 128
HALO = 32
TILE = 128
WIDTH = 2 * TILE
OBS_TILE = 256
CODE = 32512.0
MESH = pl.DeviceIdType.MESH


def mirror_rows(count):
    rows = []
    for first in range(count):
        for second in range(count):
            low = min(first, second)
            high = max(first, second)
            rows.append(low * count - low * (low - 1) // 2 + high - low)
    return rows


def padded(count, unit):
    return -(-count // unit) * unit


def peer(axis, index):
    if axis == "obs":
        return (index, lax.axis_index("chan"))
    return (lax.axis_index("obs"), index)


def kernel(n_obs, n_chan, scatter, dep, pred, inv, ids, counts, *rest):
    if scatter:
        gram_out, rhs_out = rest[:2]
        rest = rest[2:]
    else:
        part_out = rest[0]
        rest = rest[1:]
    (
        window,
        strip,
        pred_in,
        inv_in,
        ids_in,
        counts_in,
        wide,
        pairs_t,
        preds_t,
        flip,
        bands,
        turned_w,
        x_code,
        z_code,
        landed_x,
        landed_z,
        total,
        small_sem,
        load_sem,
        halo_send,
        halo_recv,
        x_send,
        x_recv,
        z_send,
        z_recv,
    ) = rest
    own, obs_dev = dep.shape
    preds = pred.shape[0]
    offsets = inv.shape[0]
    half = offsets // 2
    upper = preds * (preds + 1) // 2
    pad = padded(upper, 8)
    tall = pairs_t.shape[0]
    flat = preds_t.shape[0]
    blocks = own // WIDTH
    levels = blocks // 2
    stages = obs_dev // (2 * OBS_TILE)
    lines = counts.shape[0]
    slots = obs_dev // lines
    me = lax.axis_index("obs")
    chan = lax.axis_index("chan")
    right = lax.rem(chan + 1, n_chan)
    left = lax.rem(chan + n_chan - 1, n_chan)
    if scatter:
        col = lax.rem(me, 2)
        lev = lax.div(me, 2)
        partner = me + 1 - 2 * col
    else:
        col = 1
        lev = levels - 1
        partner = me
    early = lev == 0 if scatter else me < 0

    def level_at(turn):
        turn = jnp.int32(turn)
        return jnp.where(turn == levels - 1, lev, jnp.where(turn >= lev, turn + 1, turn))

    def level_of(step):
        step = jnp.int32(step)
        if not scatter:
            return lax.div(step, 2)
        late_first = jnp.where(step < 2, 1 - step, step)
        late_last = jnp.where(step == levels - 1, 0, step + 1)
        late_mid = jnp.where(
            step == levels - 1, levels - 1, jnp.where(step == levels - 2, 0, step + 1)
        )
        lead = jnp.where(
            early,
            jnp.where(col == 0, late_mid, late_last),
            jnp.where(col == 0, step, late_first),
        )
        return jnp.where(step < levels, lead, level_at(step - levels))

    def block_at(step):
        step = jnp.int32(step)
        if not scatter:
            return jnp.where(step < 2, 1 - step, step)
        return 2 * level_of(step) + jnp.where(step < levels, 1 - col, col)

    def chunk_at(place):
        if not scatter:
            return place
        turned_on = jnp.where(place < 3, place + 1, jnp.where(place == 3, 0, place))
        return jnp.where(
            early, lax.rem(2 - col + place, blocks), jnp.where(col == 0, place, turned_on)
        )

    barrier = pltpu.get_barrier_semaphore()
    for index in (left, right):
        pl.semaphore_signal(barrier, inc=1, device_id=peer("chan", index), device_id_type=MESH)
    greeted = 2
    if scatter:
        pl.semaphore_signal(barrier, inc=1, device_id=peer("obs", partner), device_id_type=MESH)
        for turn in range(levels - 1):
            index = 2 * level_at(turn) + col
            pl.semaphore_signal(barrier, inc=1, device_id=peer("obs", index), device_id_type=MESH)
        greeted += levels

    base = pl.multiple_of(chan * own, own)
    smalls = [
        pltpu.make_async_copy(pred, pred_in, small_sem.at[0]),
        pltpu.make_async_copy(counts, counts_in, small_sem.at[1]),
        pltpu.make_async_copy(inv, inv_in, small_sem.at[2]),
        pltpu.make_async_copy(
            ids.at[:, pl.ds(base, own)], ids_in.at[:, pl.ds(LANES, own)], small_sem.at[3]
        ),
        pltpu.make_async_copy(
            ids.at[:, pl.ds(pl.multiple_of(jnp.maximum(base - LANES, 0), LANES), LANES)],
            ids_in.at[:, pl.ds(0, LANES)],
            small_sem.at[4],
        ),
        pltpu.make_async_copy(
            ids.at[
                :, pl.ds(pl.multiple_of(jnp.minimum(base + own, own * n_chan - LANES), LANES), LANES)
            ],
            ids_in.at[:, pl.ds(LANES + own, LANES)],
            small_sem.at[5],
        ),
    ]
    for copy in smalls:
        copy.start()

    def load(place):
        chunk = chunk_at(jnp.int32(place))
        start = pl.multiple_of(chunk * WIDTH, WIDTH)
        return pltpu.make_async_copy(
            dep.at[pl.ds(start, WIDTH), :],
            window.at[pl.ds(start + HALO, WIDTH), :],
            load_sem.at[place],
        )

    strips = [
        pltpu.make_async_copy(dep.at[pl.ds(0, HALO), :], strip.at[0], small_sem.at[6]),
        pltpu.make_async_copy(dep.at[pl.ds(own - HALO, HALO), :], strip.at[1], small_sem.at[7]),
    ]
    for copy in strips:
        copy.start()
    for place in range(3):
        load(place).start()

    to_left = pltpu.make_async_remote_copy(
        src_ref=strip.at[0],
        dst_ref=window.at[pl.ds(own + HALO, HALO), :],
        send_sem=halo_send.at[0],
        recv_sem=halo_recv.at[0],
        device_id=peer("chan", left),
        device_id_type=MESH,
    )
    to_right = pltpu.make_async_remote_copy(
        src_ref=strip.at[1],
        dst_ref=window.at[pl.ds(0, HALO), :],
        send_sem=halo_send.at[1],
        recv_sem=halo_recv.at[1],
        device_id=peer("chan", right),
        device_id_type=MESH,
    )

    def meet():
        pl.semaphore_wait(barrier, greeted)
        pl.when(chan > 0)(to_left.start)
        pl.when(chan < n_chan - 1)(to_right.start)

    rim = jnp.zeros((HALO, obs_dev), window.dtype)
    window[own + 2 * HALO :, :] = jnp.zeros((window.shape[0] - own - 2 * HALO, obs_dev), window.dtype)

    @pl.when(chan == 0)
    def _():
        window[:HALO, :] = rim

    @pl.when(chan == n_chan - 1)
    def _():
        window[own + HALO : own + 2 * HALO, :] = rim

    flip[...] = jnp.zeros_like(flip)
    wide[...] = jnp.zeros_like(wide)

    smalls[0].wait()
    smalls[1].wait()
    for place in range(3, blocks):
        load(place).start()
    values = pred_in[...].astype(jnp.float32)
    first_row = 0
    for first in range(preds):
        count = preds - first
        wide[first_row : first_row + count, :] = values[first:, :] * values[first : first + 1, :]
        first_row += count
    wide[tall : tall + preds, :] = values

    def mask_line(line, carry):
        at = pl.ds(pl.multiple_of(line * slots, slots), slots)
        slot = lax.broadcasted_iota(jnp.int32, (tall + flat, slots), 1)
        live = jnp.where(slot < counts_in[line], wide[:, at], 0.0).astype(jnp.bfloat16)
        pairs_t[:, at] = live[:tall, :]
        preds_t[:, at] = live[tall:, :]
        return carry

    lax.fori_loop(0, lines, mask_line, 0, unroll=4)

    for copy in smalls[2:]:
        copy.wait()

    @pl.when(chan == 0)
    def _():
        ids_in[:, 0:LANES] = jnp.full((1, LANES), -1, jnp.int32)

    @pl.when(chan == n_chan - 1)
    def _():
        ids_in[:, LANES + own :] = jnp.full((1, LANES), -1, jnp.int32)

    def build(block, side):
        for part in range(2):
            first = pl.multiple_of(block * WIDTH + part * TILE, TILE)
            near = ids_in[:, pl.ds(first, 3 * TILE)].astype(jnp.float32)
            flip[part, 0:offsets, :] = inv_in[:, pl.ds(first, TILE)].astype(jnp.float32)
            flip[part, 64:65, :] = near[:, TILE : 2 * TILE]
            turned = flip[part].T
            own_id = turned[:, 64:65]
            place = lax.broadcasted_iota(jnp.int32, turned.shape, 1)
            turned = jnp.where(place < offsets, turned, 0.0)
            skewed = pltpu.roll(
                jnp.concatenate([turned, jnp.zeros_like(turned)], axis=1),
                HALO - half,
                1,
                stride=1,
                stride_axis=0,
            )
            same = near[:, TILE - HALO : 3 * TILE - HALO] == own_id
            bands[side, part * TILE : (part + 1) * TILE, :] = jnp.where(same, skewed, 0.0).astype(
                jnp.bfloat16
            )

    def send_x(step, level):
        return pltpu.make_async_remote_copy(
            src_ref=x_code.at[step],
            dst_ref=landed_x.at[level],
            send_sem=x_send.at[step],
            recv_sem=x_recv.at[level],
            device_id=peer("obs", partner),
            device_id_type=MESH,
        )

    def send_z(turn):
        return pltpu.make_async_remote_copy(
            src_ref=z_code.at[turn],
            dst_ref=landed_z.at[lev],
            send_sem=z_send.at[turn],
            recv_sem=z_recv.at[lev],
            device_id=peer("obs", 2 * level_at(turn) + col),
            device_id_type=MESH,
        )

    def from_z(turn):
        sender = level_at(turn)
        return pltpu.make_async_remote_copy(
            src_ref=z_code.at[0],
            dst_ref=landed_z.at[sender],
            send_sem=z_send.at[0],
            recv_sem=z_recv.at[sender],
            device_id=peer("obs", 2 * sender + col),
            device_id_type=MESH,
        )

    def encode(sums):
        gram = sums[:pad]
        rhs = sums[pad:]

        def grade(part):
            most = jnp.max(jnp.abs(part), axis=0, keepdims=True)
            return jnp.ceil(jnp.log2(jnp.maximum(most, 1e-30)))

        gram_grade = grade(gram)
        rhs_grade = grade(rhs)
        row = lax.broadcasted_iota(jnp.int32, rhs.shape, 0)
        gram = gram * (jnp.exp2(-gram_grade) * CODE)
        rhs = rhs * (jnp.exp2(-rhs_grade) * CODE)
        rhs = jnp.where(row == preds, gram_grade, rhs)
        rhs = jnp.where(row == preds + 1, rhs_grade, rhs)
        return jnp.round(jnp.concatenate([gram, rhs], axis=0)).astype(jnp.int32).astype(jnp.int16)

    def decode(code):
        values = code.astype(jnp.int32).astype(jnp.float32)
        gram_scale = jnp.exp2(values[pad + preds : pad + preds + 1]) * (1.0 / CODE)
        rhs_scale = jnp.exp2(values[pad + preds + 1 : pad + preds + 2]) * (1.0 / CODE)
        return jnp.concatenate([values[:pad] * gram_scale, values[pad:] * rhs_scale], axis=0)

    def accumulated(*accs):
        narrow = [[accs[4 * mxu + 2 * side : 4 * mxu + 2 * side + 2] for side in range(2)] for mxu in range(2)]
        tall_acc = [accs[8 + 2 * mxu : 10 + 2 * mxu] for mxu in range(2)]
        flat_acc = [accs[12 + 2 * mxu : 14 + 2 * mxu] for mxu in range(2)]

        def weigh(block, band, stage):
            start = pl.multiple_of(block * WIDTH, WIDTH)
            for mxu in range(2):
                at = (2 * stage + mxu) * OBS_TILE
                for part in range(2):
                    first = pl.multiple_of(start + part * TILE, TILE)
                    pltpu.matmul_push_rhs(
                        window[pl.ds(first, 2 * TILE), at : at + OBS_TILE],
                        staging_register=part,
                        mxu_index=mxu,
                    )
                    pltpu.matmul_acc_lhs(
                        narrow[mxu][stage % 2][part],
                        bands[band, part * TILE : (part + 1) * TILE, :],
                        load_staged_rhs=part,
                    )

        def turn_over(stage):
            for mxu in range(2):
                for part in range(2):
                    weighted = pltpu.matmul_pop(narrow[mxu][stage % 2][part])
                    turned_w[stage % 2, mxu, :, part * TILE : (part + 1) * TILE] = weighted.astype(
                        jnp.bfloat16
                    ).T

        def gather(side, stage):
            edge = jnp.bfloat16(huber_edge)
            for mxu in range(2):
                at = (2 * stage + mxu) * OBS_TILE
                weighted = turned_w[stage % 2, mxu]
                qc_weight = edge / jnp.maximum(jnp.abs(weighted), edge)
                scaled = jnp.clip(weighted, -edge, edge)
                pltpu.matmul_push_rhs(qc_weight, staging_register=0, mxu_index=mxu)
                pltpu.matmul_acc_lhs(
                    tall_acc[mxu][side], pairs_t[:, at : at + OBS_TILE], load_staged_rhs=0
                )
                pltpu.matmul_push_rhs(scaled, staging_register=1, mxu_index=mxu)
                pltpu.matmul_acc_lhs(
                    flat_acc[mxu][side], preds_t[:, at : at + OBS_TILE], load_staged_rhs=1
                )

        def result(side):
            gram = pltpu.matmul_pop(tall_acc[0][side]) + pltpu.matmul_pop(tall_acc[1][side])
            rhs = pltpu.matmul_pop(flat_acc[0][side]) + pltpu.matmul_pop(flat_acc[1][side])
            return jnp.concatenate([gram[:pad], rhs], axis=0)

        def keep(step, sums):
            start = pl.multiple_of(block_at(step) * WIDTH, WIDTH)
            part_out[:, pl.ds(start, WIDTH)] = sums

        def pass_across(step, sums):
            x_code[step] = encode(sums)
            send_x(step, level_of(step)).start()

        def joined(step, sums):
            level = level_of(step)
            send_x(0, level).wait_recv()
            return sums + decode(landed_x[level])

        def pass_along(step, sums):
            turn = step - levels
            z_code[turn] = encode(joined(step, sums))
            send_z(turn).start()

        for acc in accs:
            pltpu.matmul_pop(acc)
        build(block_at(0), 0)
        for copy in strips:
            copy.wait()
        pl.when(jnp.logical_not(early))(meet)
        for place in range(3):
            load(place).wait()
        weigh(block_at(0), 0, 0)
        weigh(block_at(0), 0, 1)
        turn_over(0)

        def one_turn(turn, carry):
            for side in range(2):
                step = 2 * turn + side
                block = block_at(step)
                following = block_at(jnp.minimum(step + 1, blocks - 1))
                more = step + 1 < blocks
                build(following, 1 - side)
                for stage in range(stages):
                    if stage == 1:
                        sums = result(1 - side)
                        places = range(3 + 2 * side, 5 + 3 * side)

                        @pl.when(turn == 0)
                        def _():
                            for place in places:
                                load(place).wait()

                        if side == 1:
                            pl.when(jnp.logical_and(early, turn == 0))(meet)

                        if scatter:

                            @pl.when(jnp.logical_and(step > 0, step <= levels))
                            def _():
                                pass_across(step - 1, sums)

                            @pl.when(step > levels)
                            def _():
                                pass_along(step - 1, sums)

                        else:

                            @pl.when(step > 0)
                            def _():
                                keep(step - 1, sums)

                        @pl.when(jnp.logical_and(more, jnp.logical_and(following == 0, chan > 0)))
                        def _():
                            to_right.wait_recv()

                        @pl.when(
                            jnp.logical_and(
                                more,
                                jnp.logical_and(following == blocks - 1, chan < n_chan - 1),
                            )
                        )
                        def _():
                            to_left.wait_recv()

                    ahead = stage + 2
                    if ahead < stages:
                        weigh(block, side, ahead)
                    else:
                        weigh(following, 1 - side, ahead - stages)
                    turn_over((stage + 1) % stages)
                    gather(side, stage)
            return carry

        lax.fori_loop(0, levels, one_turn, 0)
        for mxu in range(2):
            for part in range(2):
                for side in range(2):
                    pltpu.matmul_pop(narrow[mxu][side][part])
        sums = result(1)
        pl.when(chan > 0)(to_left.wait_send)
        pl.when(chan < n_chan - 1)(to_right.wait_send)
        if not scatter:
            keep(blocks - 1, sums)
            return
        sums = joined(blocks - 1, sums)
        for turn in range(levels - 1):
            from_z(turn).wait_recv()
            sums = sums + decode(landed_z[level_at(turn)])
        total[...] = sums * (1.0 / float(obs_dev * n_obs))
        for row, source in enumerate(mirror_rows(preds)):
            gram_out[row : row + 1, :] = total[source : source + 1, :]
        rhs_out[...] = total[pad : pad + preds, :]
        for step in range(levels):
            send_x(step, 0).wait_send()
        for turn in range(levels - 1):
            send_z(turn).wait_send()

    pl.run_scoped(accumulated, *acc_list(tall, flat))


def acc_list(tall, flat):
    specs = []
    for rows, copies in ((TILE, 4), (tall, 2), (flat, 2)):
        for mxu in range(2):
            specs += [pltpu.ACC(mxu)((rows, OBS_TILE), jnp.float32)] * copies
    return specs


def on_device(departures, predictors, inv_band, band_id, line_counts):
    own, obs_dev = departures.shape
    preds = predictors.shape[0]
    upper = preds * (preds + 1) // 2
    n_obs = lax.axis_size("obs")
    n_chan = lax.axis_size("chan")
    share = own // n_obs
    blocks = own // WIDTH
    scatter = share == WIDTH and n_obs % 2 == 0 and n_obs >= 8
    pad = padded(upper, 8)
    tall = padded(upper, 16)
    flat = padded(preds + 2, 16)
    rows = pad + flat
    if scatter:
        out_shape = (
            pltpu.VMEM((preds * preds, share), jnp.float32),
            pltpu.VMEM((preds, share), jnp.float32),
        )
    else:
        out_shape = (jax.ShapeDtypeStruct((rows, own), jnp.float32),)
    vmem = pl.BlockSpec(memory_space=pltpu.VMEM)
    hbm = pl.BlockSpec(memory_space=pltpu.HBM)
    levels = blocks // 2
    kept = (levels, rows, WIDTH) if scatter else (1, 8, LANES)
    dma = pltpu.SemaphoreType.DMA
    outs = pl.pallas_call(
        functools.partial(kernel, n_obs, n_chan, scatter),
        out_shape=out_shape,
        in_specs=[hbm] * 5,
        out_specs=tuple(vmem for _ in out_shape),
        scratch_shapes=[
            pltpu.VMEM((own + 4 * HALO, obs_dev), jnp.bfloat16),
            pltpu.VMEM((2, HALO, obs_dev), jnp.bfloat16),
            pltpu.VMEM(predictors.shape, jnp.bfloat16),
            pltpu.VMEM(inv_band.shape, jnp.bfloat16),
            pltpu.VMEM((1, own + 2 * LANES), jnp.int32),
            pltpu.SMEM(line_counts.shape, jnp.int32),
            pltpu.VMEM((tall + flat, obs_dev), jnp.float32),
            pltpu.VMEM((tall, obs_dev), jnp.bfloat16),
            pltpu.VMEM((flat, obs_dev), jnp.bfloat16),
            pltpu.VMEM((2, LANES, TILE), jnp.float32),
            pltpu.VMEM((2, WIDTH, 2 * TILE), jnp.bfloat16),
            pltpu.VMEM((2, 2, OBS_TILE, WIDTH), jnp.bfloat16),
            pltpu.VMEM(kept, jnp.int16),
            pltpu.VMEM(kept, jnp.int16),
            pltpu.VMEM(kept, jnp.int16),
            pltpu.VMEM(kept, jnp.int16),
            pltpu.VMEM((rows, WIDTH), jnp.float32),
            dma((8,)),
            dma((blocks,)),
            dma((2,)),
            dma((2,)),
            dma((levels,)),
            dma((levels,)),
            dma((levels,)),
            dma((levels,)),
        ],
        compiler_params=pltpu.CompilerParams(
            collective_id=0,
            has_side_effects=True,
            vmem_limit_bytes=67043328 - 120 * 1024,
        ),
        name="normal_equations",
    )(departures, predictors, inv_band, band_id[None, :], line_counts)
    if scatter:
        return outs[0], outs[1]
    factor = 1.0 / float(obs_dev * n_obs)
    part = lax.psum_scatter(outs[0], "obs", scatter_dimension=1, tiled=True) * factor
    mirror = np.array(mirror_rows(preds))
    return part[mirror], part[pad : pad + preds]


def solution(mesh):
    in_specs = (P("chan", "obs"), P(None, "obs"), P(None, "chan"), P(), P("obs"))
    out_specs = (P(None, ("chan", "obs")), P(None, ("chan", "obs")))
    return jax.shard_map(
        on_device, mesh=mesh, in_specs=in_specs, out_specs=out_specs, check_vma=False
    )
```

```python
import functools

import jax
import jax.numpy as jnp
import numpy as np
from jax import lax
from jax.experimental import pallas as pl
from jax.experimental.pallas import tpu as pltpu
from jax.sharding import PartitionSpec as P

huber_edge = 1.0
LANES = 128
HALO = 32
TILE = 128
WIDTH = 2 * TILE
OBS_TILE = 256
CODE = 32512.0
MESH = pl.DeviceIdType.MESH


def mirror_rows(count):
    rows = []
    for first in range(count):
        for second in range(count):
            low = min(first, second)
            high = max(first, second)
            rows.append(low * count - low * (low - 1) // 2 + high - low)
    return rows


def padded(count, unit):
    return -(-count // unit) * unit


def peer(axis, index):
    if axis == "obs":
        return (index, lax.axis_index("chan"))
    return (lax.axis_index("obs"), index)


def kernel(n_obs, n_chan, scatter, dep, pred, inv, ids, counts, *rest):
    if scatter:
        gram_out, rhs_out = rest[:2]
        rest = rest[2:]
    else:
        part_out = rest[0]
        rest = rest[1:]
    (
        window,
        strip,
        pred_in,
        inv_in,
        ids_in,
        counts_in,
        wide,
        pairs_t,
        preds_t,
        flip,
        spun,
        bands,
        turned_w,
        mine,
        x_code,
        z_code,
        d_code,
        landed_x,
        landed_z,
        landed_d,
        total,
        small_sem,
        load_sem,
        halo_send,
        halo_recv,
        x_send,
        x_recv,
        z_send,
        z_recv,
        d_send,
        d_recv,
    ) = rest
    own, obs_dev = dep.shape
    preds = pred.shape[0]
    offsets = inv.shape[0]
    half = offsets // 2
    upper = preds * (preds + 1) // 2
    pad = padded(upper, 8)
    tall = pairs_t.shape[1]
    flat = preds_t.shape[1]
    blocks = own // WIDTH
    levels = blocks // 2
    stages = obs_dev // (2 * OBS_TILE)
    lines = counts.shape[0]
    slots = obs_dev // lines
    me = lax.axis_index("obs")
    chan = lax.axis_index("chan")
    right = lax.rem(chan + 1, n_chan)
    left = lax.rem(chan + n_chan - 1, n_chan)
    if scatter:
        col = lax.rem(me, 2)
        lev = lax.div(me, 2)
        partner = me + 1 - 2 * col
    else:
        col = 1
        lev = levels - 1
        partner = me
    early = lev == 0 if scatter else me < 0

    def is_any(step, choices):
        found = step == choices[0]
        for choice in choices[1:]:
            found = jnp.logical_or(found, step == choice)
        return found

    def straight(step):
        return jnp.logical_or(early, is_any(step, (0, 2)))

    def across(step):
        return jnp.logical_and(jnp.logical_not(early), is_any(step, (1, 3, 4)))

    def level_across(step):
        return jnp.where(step < 2, 1, step - 1)

    def level_at(turn):
        shifted = jnp.where(turn + 1 >= lev, turn + 2, turn + 1)
        return jnp.where(turn == levels - 2, lev, shifted)

    def turn_along(step):
        return step - 5

    def block_at(step):
        step = jnp.int32(step)
        if not scatter:
            return jnp.where(step < 2, 1 - step, step)
        ahead = jnp.where(step == 4, 1, jnp.where(step < 4, step + 2, step + 1))
        ahead = jnp.where(step == 5, 0, jnp.where(step > 5, step, ahead))
        later = jnp.where(
            is_any(step, (0, 2)),
            jnp.where(step == 0, 1, 0),
            jnp.where(
                is_any(step, (1, 3, 4)),
                2 * level_across(step) + 1 - col,
                2 * level_at(turn_along(step)) + col,
            ),
        )
        return jnp.where(early, ahead, later)

    def chunk_at(place):
        if not scatter:
            return place
        return jnp.where(early, lax.rem(place + 1, blocks), place)

    barrier = pltpu.get_barrier_semaphore()
    for index in (left, right):
        pl.semaphore_signal(barrier, inc=1, device_id=peer("chan", index), device_id_type=MESH)
    greeted = 2
    if scatter:
        pl.semaphore_signal(barrier, inc=1, device_id=peer("obs", partner), device_id_type=MESH)
        for away in range(1, levels):
            index = 2 * lax.rem(lev + away, levels) + col
            pl.semaphore_signal(barrier, inc=1, device_id=peer("obs", index), device_id_type=MESH)

        @pl.when(early)
        def _():
            for level in range(1, levels):
                index = 2 * level + 1 - col
                pl.semaphore_signal(
                    barrier, inc=1, device_id=peer("obs", index), device_id_type=MESH
                )

        @pl.when(jnp.logical_not(early))
        def _():
            pl.semaphore_signal(barrier, inc=1, device_id=peer("obs", 1 - col), device_id_type=MESH)

        greeted += levels + jnp.where(early, levels - 1, 1)

    base = pl.multiple_of(chan * own, own)
    smalls = [
        pltpu.make_async_copy(pred, pred_in, small_sem.at[0]),
        pltpu.make_async_copy(counts, counts_in, small_sem.at[1]),
        pltpu.make_async_copy(inv, inv_in, small_sem.at[2]),
        pltpu.make_async_copy(
            ids.at[:, pl.ds(base, own)], ids_in.at[:, pl.ds(LANES, own)], small_sem.at[3]
        ),
        pltpu.make_async_copy(
            ids.at[:, pl.ds(pl.multiple_of(jnp.maximum(base - LANES, 0), LANES), LANES)],
            ids_in.at[:, pl.ds(0, LANES)],
            small_sem.at[4],
        ),
        pltpu.make_async_copy(
            ids.at[
                :, pl.ds(pl.multiple_of(jnp.minimum(base + own, own * n_chan - LANES), LANES), LANES)
            ],
            ids_in.at[:, pl.ds(LANES + own, LANES)],
            small_sem.at[5],
        ),
    ]
    for copy in smalls[:2]:
        copy.start()

    def load(place):
        chunk = chunk_at(jnp.int32(place))
        start = pl.multiple_of(chunk * WIDTH, WIDTH)
        return pltpu.make_async_copy(
            dep.at[pl.ds(start, WIDTH), :],
            window.at[pl.ds(start + HALO, WIDTH), :],
            load_sem.at[place],
        )

    strips = [
        pltpu.make_async_copy(dep.at[pl.ds(0, HALO), :], strip.at[0], small_sem.at[6]),
        pltpu.make_async_copy(dep.at[pl.ds(own - HALO, HALO), :], strip.at[1], small_sem.at[7]),
    ]
    for copy in strips + smalls[2:]:
        copy.start()
    for place in range(3):
        load(place).start()

    to_left = pltpu.make_async_remote_copy(
        src_ref=strip.at[0],
        dst_ref=window.at[pl.ds(own + HALO, HALO), :],
        send_sem=halo_send.at[0],
        recv_sem=halo_recv.at[0],
        device_id=peer("chan", left),
        device_id_type=MESH,
    )
    to_right = pltpu.make_async_remote_copy(
        src_ref=strip.at[1],
        dst_ref=window.at[pl.ds(0, HALO), :],
        send_sem=halo_send.at[1],
        recv_sem=halo_recv.at[1],
        device_id=peer("chan", right),
        device_id_type=MESH,
    )

    def meet():
        pl.semaphore_wait(barrier, greeted)
        pl.when(chan > 0)(to_left.start)
        pl.when(chan < n_chan - 1)(to_right.start)

    rim = jnp.zeros((HALO, obs_dev), window.dtype)
    window[own + 2 * HALO :, :] = jnp.zeros((window.shape[0] - own - 2 * HALO, obs_dev), window.dtype)

    @pl.when(chan == 0)
    def _():
        window[:HALO, :] = rim

    @pl.when(chan == n_chan - 1)
    def _():
        window[own + HALO : own + 2 * HALO, :] = rim

    flip[...] = jnp.zeros_like(flip)
    wide[...] = jnp.zeros_like(wide)

    smalls[0].wait()
    smalls[1].wait()
    values = pred_in[...].astype(jnp.float32)
    first_row = 0
    for first in range(preds):
        count = preds - first
        wide[first_row : first_row + count, :] = values[first:, :] * values[first : first + 1, :]
        first_row += count
    wide[tall : tall + preds, :] = values

    def mask_line(line, carry):
        at = pl.ds(pl.multiple_of(line * slots, slots), slots)
        slot = lax.broadcasted_iota(jnp.int32, (tall + flat, slots), 1)
        live = jnp.where(slot < counts_in[line], wide[:, at], 0.0).astype(jnp.bfloat16)
        pairs_t[line] = live[:tall, :]
        preds_t[line] = live[tall:, :]
        return carry

    lax.fori_loop(0, lines, mask_line, 0, unroll=4)

    for copy in strips + smalls[2:]:
        copy.wait()
    for place in range(3, 5):
        load(place).start()

    @pl.when(chan == 0)
    def _():
        ids_in[:, 0:LANES] = jnp.full((1, LANES), -1, jnp.int32)

    @pl.when(chan == n_chan - 1)
    def _():
        ids_in[:, LANES + own :] = jnp.full((1, LANES), -1, jnp.int32)

    def turn_band(block):
        for part in range(2):
            first = pl.multiple_of(block * WIDTH + part * TILE, TILE)
            own_ids = ids_in[:, pl.ds(first + TILE, TILE)].astype(jnp.float32)
            flip[part, 0:offsets, :] = inv_in[:, pl.ds(first, TILE)].astype(jnp.float32)
            flip[part, 64:65, :] = own_ids
            spun[part] = flip[part].T

    def skew_band(block, side):
        for part in range(2):
            first = pl.multiple_of(block * WIDTH + part * TILE, TILE)
            near = ids_in[:, pl.ds(first, 3 * TILE)].astype(jnp.float32)
            turned = spun[part]
            own_id = turned[:, 64:65]
            place = lax.broadcasted_iota(jnp.int32, turned.shape, 1)
            turned = jnp.where(place < offsets, turned, 0.0)
            skewed = pltpu.roll(
                jnp.concatenate([turned, jnp.zeros_like(turned)], axis=1),
                HALO - half,
                1,
                stride=1,
                stride_axis=0,
            )
            same = near[:, TILE - HALO : 3 * TILE - HALO] == own_id
            band = jnp.where(same, skewed, 0.0).astype(jnp.bfloat16)
            bands[side, part, 0] = band[:, :LANES]
            bands[side, part, 1] = band[:, LANES:]

    def wide_of(ref, first, second):
        return jnp.concatenate([ref[first, second, 0], ref[first, second, 1]], axis=1)

    def paired(ref, at):
        return jnp.concatenate([ref[at // LANES], ref[at // LANES + 1]], axis=1)

    def send_x(level):
        return pltpu.make_async_remote_copy(
            src_ref=x_code.at[level],
            dst_ref=landed_x.at[level],
            send_sem=x_send.at[level],
            recv_sem=x_recv.at[level],
            device_id=peer("obs", partner),
            device_id_type=MESH,
        )

    def send_z(level):
        return pltpu.make_async_remote_copy(
            src_ref=z_code.at[level],
            dst_ref=landed_z.at[lev],
            send_sem=z_send.at[level],
            recv_sem=z_recv.at[lev],
            device_id=peer("obs", 2 * level + col),
            device_id_type=MESH,
        )

    def from_z(level):
        return pltpu.make_async_remote_copy(
            src_ref=z_code.at[0],
            dst_ref=landed_z.at[level],
            send_sem=z_send.at[0],
            recv_sem=z_recv.at[level],
            device_id=peer("obs", 2 * level + col),
            device_id_type=MESH,
        )

    def send_straight(block):
        return pltpu.make_async_remote_copy(
            src_ref=d_code.at[block],
            dst_ref=landed_d.at[me],
            send_sem=d_send.at[block],
            recv_sem=d_recv.at[me],
            device_id=peer("obs", block),
            device_id_type=MESH,
        )

    def from_straight(source):
        return pltpu.make_async_remote_copy(
            src_ref=d_code.at[0],
            dst_ref=landed_d.at[source],
            send_sem=d_send.at[0],
            recv_sem=d_recv.at[source],
            device_id=peer("obs", source),
            device_id_type=MESH,
        )

    def encode(sums):
        gram = sums[:pad]
        rhs = sums[pad:]

        def grade(part):
            most = jnp.max(jnp.abs(part), axis=0, keepdims=True)
            return jnp.ceil(jnp.log2(jnp.maximum(most, 1e-30)))

        gram_grade = grade(gram)
        rhs_grade = grade(rhs)
        row = lax.broadcasted_iota(jnp.int32, rhs.shape, 0)
        gram = gram * (jnp.exp2(-gram_grade) * CODE)
        rhs = rhs * (jnp.exp2(-rhs_grade) * CODE)
        rhs = jnp.where(row == preds, gram_grade, rhs)
        rhs = jnp.where(row == preds + 1, rhs_grade, rhs)
        return jnp.round(jnp.concatenate([gram, rhs], axis=0)).astype(jnp.int32).astype(jnp.int16)

    def decode(code):
        values = code.astype(jnp.int32).astype(jnp.float32)
        gram_scale = jnp.exp2(values[pad + preds : pad + preds + 1]) * (1.0 / CODE)
        rhs_scale = jnp.exp2(values[pad + preds + 1 : pad + preds + 2]) * (1.0 / CODE)
        return jnp.concatenate([values[:pad] * gram_scale, values[pad:] * rhs_scale], axis=0)

    def accumulated(*accs):
        narrow = [[accs[4 * mxu + 2 * side : 4 * mxu + 2 * side + 2] for side in range(2)] for mxu in range(2)]
        tall_acc = [accs[8 + 2 * mxu : 10 + 2 * mxu] for mxu in range(2)]
        flat_acc = [accs[12 + 2 * mxu : 14 + 2 * mxu] for mxu in range(2)]

        def weigh(block, band, stage):
            start = pl.multiple_of(block * WIDTH, WIDTH)
            for mxu in range(2):
                at = (2 * stage + mxu) * OBS_TILE
                for part in range(2):
                    first = pl.multiple_of(start + part * TILE, TILE)
                    pltpu.matmul_push_rhs(
                        window[pl.ds(first, 2 * TILE), at : at + OBS_TILE],
                        staging_register=part,
                        mxu_index=mxu,
                    )
                    pltpu.matmul_acc_lhs(
                        narrow[mxu][stage % 2][part],
                        wide_of(bands, band, part),
                        load_staged_rhs=part,
                    )

        def turn_over(stage):
            for mxu in range(2):
                for part in range(2):
                    weighted = pltpu.matmul_pop(narrow[mxu][stage % 2][part])
                    turned_w[stage % 4, mxu, part] = weighted.astype(jnp.bfloat16).T

        def gather(side, stage):
            edge = jnp.bfloat16(huber_edge)
            for mxu in range(2):
                at = (2 * stage + mxu) * OBS_TILE
                weighted = wide_of(turned_w, stage % 4, mxu)
                qc_weight = edge / jnp.maximum(jnp.abs(weighted), edge)
                scaled = jnp.clip(weighted, -edge, edge)
                pltpu.matmul_push_rhs(qc_weight, staging_register=0, mxu_index=mxu)
                pltpu.matmul_acc_lhs(
                    tall_acc[mxu][side], paired(pairs_t, at), load_staged_rhs=0
                )
                pltpu.matmul_push_rhs(scaled, staging_register=1, mxu_index=mxu)
                pltpu.matmul_acc_lhs(
                    flat_acc[mxu][side], paired(preds_t, at), load_staged_rhs=1
                )

        def result(side):
            gram = pltpu.matmul_pop(tall_acc[0][side]) + pltpu.matmul_pop(tall_acc[1][side])
            rhs = pltpu.matmul_pop(flat_acc[0][side]) + pltpu.matmul_pop(flat_acc[1][side])
            return jnp.concatenate([gram[:pad], rhs], axis=0)

        def keep(step, sums):
            start = pl.multiple_of(block_at(step) * WIDTH, WIDTH)
            part_out[:, pl.ds(start, WIDTH)] = sums

        def joined(step, sums):
            level = level_at(turn_along(step))
            send_x(level).wait_recv()
            return sums + decode(landed_x[level])

        def pass_along(step, sums):
            level = level_at(turn_along(step))
            z_code[level] = encode(joined(step, sums))
            send_z(level).start()

        def deliver(step, sums):
            block = block_at(step)
            own_block = jnp.logical_and(early, block == col)

            @pl.when(jnp.logical_and(straight(step), own_block))
            def _():
                mine[...] = sums

            @pl.when(jnp.logical_and(straight(step), jnp.logical_not(own_block)))
            def _():
                d_code[block] = encode(sums)
                send_straight(block).start()

            @pl.when(across(step))
            def _():
                level = level_across(step)
                x_code[level] = encode(sums)
                send_x(level).start()

            @pl.when(jnp.logical_not(jnp.logical_or(straight(step), across(step))))
            def _():
                pass_along(step, sums)

        for acc in accs:
            pltpu.matmul_pop(acc)
        turn_band(block_at(0))
        skew_band(block_at(0), 0)
        pl.when(jnp.logical_not(early))(meet)
        for place in range(5, blocks):
            load(place).start()
        turned_w[2:] = jnp.zeros((2,) + turned_w.shape[1:], turned_w.dtype)
        for place in range(3):
            load(place).wait()
        def half_step(block, side, half_at):
            for stage in (2 * half_at, 2 * half_at + 1):
                weigh(block, side, stage)
            for stage in (2 * half_at, 2 * half_at + 1):
                if half_at == 0:
                    gather(1 - side, stages - 2 + stage)
                else:
                    gather(side, stage - 2)
            for stage in (2 * half_at, 2 * half_at + 1):
                turn_over(stage)

        def one_turn(turn, carry):
            for side in range(2):
                step = 2 * turn + side
                block = block_at(step)
                following = block_at(jnp.minimum(step + 1, blocks - 1))
                more = step + 1 < blocks
                turn_band(following)
                half_step(block, side, 0)
                sums = result(1 - side)
                places = range(3 + 2 * side, 5 + 3 * side)

                @pl.when(turn == 0)
                def _():
                    for place in places:
                        load(place).wait()

                if side == 1:
                    pl.when(jnp.logical_and(early, turn == 0))(meet)

                @pl.when(step > 0)
                def _():
                    if scatter:
                        deliver(step - 1, sums)
                    else:
                        keep(step - 1, sums)

                @pl.when(jnp.logical_and(more, jnp.logical_and(following == 0, chan > 0)))
                def _():
                    to_right.wait_recv()

                @pl.when(
                    jnp.logical_and(
                        more,
                        jnp.logical_and(following == blocks - 1, chan < n_chan - 1),
                    )
                )
                def _():
                    to_left.wait_recv()

                for half_at in range(1, stages // 2):
                    half_step(block, side, half_at)
                skew_band(following, 1 - side)
            return carry

        lax.fori_loop(0, levels, one_turn, 0)
        for stage in range(stages - 2, stages):
            gather(1, stage)
        sums = result(1)
        pl.when(chan > 0)(to_left.wait_send)
        pl.when(chan < n_chan - 1)(to_right.wait_send)
        if not scatter:
            keep(blocks - 1, sums)
            return

        def finish(sums):
            total[...] = sums * (1.0 / float(obs_dev * n_obs))
            for row, source in enumerate(mirror_rows(preds)):
                gram_out[row : row + 1, :] = total[source : source + 1, :]
            rhs_out[...] = total[pad : pad + preds, :]

        @pl.when(early)
        def _():
            deliver(blocks - 1, sums)
            whole = mine[...]
            for away in range(1, n_obs):
                source = lax.rem(me + away, n_obs)
                from_straight(source).wait_recv()
                whole = whole + decode(landed_d[source])
            finish(whole)
            for away in range(1, n_obs):
                send_straight(lax.rem(me + away, n_obs)).wait_send()

        @pl.when(jnp.logical_not(early))
        def _():
            whole = joined(blocks - 1, sums)
            for source in range(2):
                from_straight(source).wait_recv()
                whole = whole + decode(landed_d[source])
            for turn in range(levels - 2):
                level = level_at(turn)
                from_z(level).wait_recv()
                whole = whole + decode(landed_z[level])
            finish(whole)
            for block in range(2):
                send_straight(block).wait_send()
            for turn in range(levels - 2):
                send_z(level_at(turn)).wait_send()
            for level in range(1, levels):
                send_x(level).wait_send()

    pl.run_scoped(accumulated, *acc_list(tall, flat))


def acc_list(tall, flat):
    specs = []
    for rows, copies in ((TILE, 4), (tall, 2), (flat, 2)):
        for mxu in range(2):
            specs += [pltpu.ACC(mxu)((rows, OBS_TILE), jnp.float32)] * copies
    return specs


def on_device(departures, predictors, inv_band, band_id, line_counts):
    own, obs_dev = departures.shape
    preds = predictors.shape[0]
    upper = preds * (preds + 1) // 2
    n_obs = lax.axis_size("obs")
    n_chan = lax.axis_size("chan")
    share = own // n_obs
    blocks = own // WIDTH
    scatter = share == WIDTH and n_obs == 8
    pad = padded(upper, 8)
    tall = padded(upper, 16)
    flat = padded(preds + 2, 16)
    rows = pad + flat
    if scatter:
        out_shape = (
            pltpu.VMEM((preds * preds, share), jnp.float32),
            pltpu.VMEM((preds, share), jnp.float32),
        )
    else:
        out_shape = (jax.ShapeDtypeStruct((rows, own), jnp.float32),)
    vmem = pl.BlockSpec(memory_space=pltpu.VMEM)
    hbm = pl.BlockSpec(memory_space=pltpu.HBM)
    levels = blocks // 2
    kept = (levels, rows, WIDTH) if scatter else (1, 8, LANES)
    many = (n_obs,) + kept[1:] if scatter else kept
    dma = pltpu.SemaphoreType.DMA
    outs = pl.pallas_call(
        functools.partial(kernel, n_obs, n_chan, scatter),
        out_shape=out_shape,
        in_specs=[hbm] * 5,
        out_specs=tuple(vmem for _ in out_shape),
        scratch_shapes=[
            pltpu.VMEM((own + 4 * HALO, obs_dev), jnp.bfloat16),
            pltpu.VMEM((2, HALO, obs_dev), jnp.bfloat16),
            pltpu.VMEM(predictors.shape, jnp.bfloat16),
            pltpu.VMEM(inv_band.shape, jnp.bfloat16),
            pltpu.VMEM((1, own + 2 * LANES), jnp.int32),
            pltpu.SMEM(line_counts.shape, jnp.int32),
            pltpu.VMEM((tall + flat, obs_dev), jnp.float32),
            pltpu.VMEM((obs_dev // LANES, tall, LANES), jnp.bfloat16),
            pltpu.VMEM((obs_dev // LANES, flat, LANES), jnp.bfloat16),
            pltpu.VMEM((2, LANES, TILE), jnp.float32),
            pltpu.VMEM((2, TILE, LANES), jnp.float32),
            pltpu.VMEM((2, 2, 2, TILE, LANES), jnp.bfloat16),
            pltpu.VMEM((4, 2, 2, OBS_TILE, LANES), jnp.bfloat16),
            pltpu.VMEM((rows, WIDTH), jnp.float32),
            pltpu.VMEM(kept, jnp.int16),
            pltpu.VMEM(kept, jnp.int16),
            pltpu.VMEM(many, jnp.int16),
            pltpu.VMEM(kept, jnp.int16),
            pltpu.VMEM(kept, jnp.int16),
            pltpu.VMEM(many, jnp.int16),
            pltpu.VMEM((rows, WIDTH), jnp.float32),
            dma((8,)),
            dma((blocks,)),
            dma((2,)),
            dma((2,)),
            dma((levels,)),
            dma((levels,)),
            dma((levels,)),
            dma((levels,)),
            dma((n_obs,)),
            dma((n_obs,)),
        ],
        compiler_params=pltpu.CompilerParams(
            collective_id=0,
            has_side_effects=True,
            vmem_limit_bytes=67043328 - 120 * 1024,
        ),
        name="normal_equations",
    )(departures, predictors, inv_band, band_id[None, :], line_counts)
    if scatter:
        return outs[0], outs[1]
    factor = 1.0 / float(obs_dev * n_obs)
    part = lax.psum_scatter(outs[0], "obs", scatter_dimension=1, tiled=True) * factor
    mirror = np.array(mirror_rows(preds))
    return part[mirror], part[pad : pad + preds]


def solution(mesh):
    in_specs = (P("chan", "obs"), P(None, "obs"), P(None, "chan"), P(), P("obs"))
    out_specs = (P(None, ("chan", "obs")), P(None, ("chan", "obs")))
    return jax.shard_map(
        on_device, mesh=mesh, in_specs=in_specs, out_specs=out_specs, check_vma=False
    )
```

```python
import functools

import jax
import jax.numpy as jnp
import numpy as np
from jax import lax
from jax.experimental import pallas as pl
from jax.experimental.pallas import tpu as pltpu
from jax.sharding import PartitionSpec as P

huber_edge = 1.0
LANES = 128
HALO = 32
TILE = 128
WIDTH = 2 * TILE
OBS_TILE = 256
CODE = 32512.0
MESH = pl.DeviceIdType.MESH


def mirror_rows(count):
    rows = []
    for first in range(count):
        for second in range(count):
            low = min(first, second)
            high = max(first, second)
            rows.append(low * count - low * (low - 1) // 2 + high - low)
    return rows


def padded(count, unit):
    return -(-count // unit) * unit


def peer(axis, index):
    if axis == "obs":
        return (index, lax.axis_index("chan"))
    return (lax.axis_index("obs"), index)


def kernel(n_obs, n_chan, scatter, dep, pred, inv, ids, counts, *rest):
    part_out = rest[0]
    rest = rest[1:]
    (
        window,
        strip,
        pred_in,
        inv_in,
        ids_in,
        counts_in,
        wide,
        pairs_t,
        preds_t,
        flip,
        spun,
        bands,
        turned_w,
        mine,
        x_code,
        z_code,
        d_code,
        landed_x,
        landed_z,
        landed_d,
        small_sem,
        load_sem,
        halo_send,
        halo_recv,
        x_send,
        x_recv,
        z_send,
        z_recv,
        d_send,
        d_recv,
    ) = rest
    own, obs_dev = dep.shape
    preds = pred.shape[0]
    offsets = inv.shape[0]
    half = offsets // 2
    upper = preds * (preds + 1) // 2
    pad = padded(upper, 8)
    tall = pairs_t.shape[1]
    flat = preds_t.shape[1]
    blocks = own // WIDTH
    levels = blocks // 2
    stages = obs_dev // (2 * OBS_TILE)
    lines = counts.shape[0]
    slots = obs_dev // lines
    me = lax.axis_index("obs")
    chan = lax.axis_index("chan")
    right = lax.rem(chan + 1, n_chan)
    left = lax.rem(chan + n_chan - 1, n_chan)
    if scatter:
        col = lax.rem(me, 2)
        lev = lax.div(me, 2)
        partner = me + 1 - 2 * col
    else:
        col = 1
        lev = levels - 1
        partner = me
    early = lev == 0 if scatter else me < 0

    def is_any(step, choices):
        found = step == choices[0]
        for choice in choices[1:]:
            found = jnp.logical_or(found, step == choice)
        return found

    def straight(step):
        return jnp.logical_or(early, is_any(step, (0, 2)))

    def across(step):
        return jnp.logical_and(jnp.logical_not(early), is_any(step, (1, 3, 4)))

    def level_across(step):
        return jnp.where(step < 2, 1, step - 1)

    def level_at(turn):
        shifted = jnp.where(turn + 1 >= lev, turn + 2, turn + 1)
        return jnp.where(turn == levels - 2, lev, shifted)

    def turn_along(step):
        return step - 5

    def block_at(step):
        step = jnp.int32(step)
        if not scatter:
            return jnp.where(step < 2, 1 - step, step)
        ahead = jnp.where(step == 4, 1, jnp.where(step < 4, step + 2, step + 1))
        ahead = jnp.where(step == 5, 0, jnp.where(step > 5, step, ahead))
        later = jnp.where(
            is_any(step, (0, 2)),
            jnp.where(step == 0, 1, 0),
            jnp.where(
                is_any(step, (1, 3, 4)),
                2 * level_across(step) + 1 - col,
                2 * level_at(turn_along(step)) + col,
            ),
        )
        return jnp.where(early, ahead, later)

    def chunk_at(place):
        if not scatter:
            return place
        return jnp.where(early, lax.rem(place + 1, blocks), place)

    barrier = pltpu.get_barrier_semaphore()
    for index in (left, right):
        pl.semaphore_signal(barrier, inc=1, device_id=peer("chan", index), device_id_type=MESH)
    greeted = 2
    if scatter:
        pl.semaphore_signal(barrier, inc=1, device_id=peer("obs", partner), device_id_type=MESH)
        for away in range(1, levels):
            index = 2 * lax.rem(lev + away, levels) + col
            pl.semaphore_signal(barrier, inc=1, device_id=peer("obs", index), device_id_type=MESH)

        @pl.when(early)
        def _():
            for level in range(1, levels):
                index = 2 * level + 1 - col
                pl.semaphore_signal(
                    barrier, inc=1, device_id=peer("obs", index), device_id_type=MESH
                )

        @pl.when(jnp.logical_not(early))
        def _():
            pl.semaphore_signal(barrier, inc=1, device_id=peer("obs", 1 - col), device_id_type=MESH)

        greeted += levels + jnp.where(early, levels - 1, 1)

    base = pl.multiple_of(chan * own, own)
    smalls = [
        pltpu.make_async_copy(pred, pred_in, small_sem.at[0]),
        pltpu.make_async_copy(counts, counts_in, small_sem.at[1]),
        pltpu.make_async_copy(inv, inv_in, small_sem.at[2]),
        pltpu.make_async_copy(
            ids.at[:, pl.ds(base, own)], ids_in.at[:, pl.ds(LANES, own)], small_sem.at[3]
        ),
        pltpu.make_async_copy(
            ids.at[:, pl.ds(pl.multiple_of(jnp.maximum(base - LANES, 0), LANES), LANES)],
            ids_in.at[:, pl.ds(0, LANES)],
            small_sem.at[4],
        ),
        pltpu.make_async_copy(
            ids.at[
                :, pl.ds(pl.multiple_of(jnp.minimum(base + own, own * n_chan - LANES), LANES), LANES)
            ],
            ids_in.at[:, pl.ds(LANES + own, LANES)],
            small_sem.at[5],
        ),
    ]
    for copy in smalls[:2]:
        copy.start()

    fore = obs_dev // stages * 2

    def load(place, part):
        chunk = chunk_at(jnp.int32(place))
        start = pl.multiple_of(chunk * WIDTH, WIDTH)
        at = pl.ds(0, fore) if part == 0 else pl.ds(fore, obs_dev - fore)
        return pltpu.make_async_copy(
            dep.at[pl.ds(start, WIDTH), at],
            window.at[pl.ds(start + HALO, WIDTH), at],
            load_sem.at[part, place],
        )

    strips = [
        pltpu.make_async_copy(dep.at[pl.ds(0, HALO), :], strip.at[0], small_sem.at[6]),
        pltpu.make_async_copy(dep.at[pl.ds(own - HALO, HALO), :], strip.at[1], small_sem.at[7]),
    ]
    for copy in strips + smalls[2:]:
        copy.start()
    for place in range(3):
        load(place, 0).start()

    to_left = pltpu.make_async_remote_copy(
        src_ref=strip.at[0],
        dst_ref=window.at[pl.ds(own + HALO, HALO), :],
        send_sem=halo_send.at[0],
        recv_sem=halo_recv.at[0],
        device_id=peer("chan", left),
        device_id_type=MESH,
    )
    to_right = pltpu.make_async_remote_copy(
        src_ref=strip.at[1],
        dst_ref=window.at[pl.ds(0, HALO), :],
        send_sem=halo_send.at[1],
        recv_sem=halo_recv.at[1],
        device_id=peer("chan", right),
        device_id_type=MESH,
    )

    def meet():
        pl.semaphore_wait(barrier, greeted)
        pl.when(chan > 0)(to_left.start)
        pl.when(chan < n_chan - 1)(to_right.start)

    rim = jnp.zeros((HALO, obs_dev), window.dtype)
    window[own + 2 * HALO :, :] = jnp.zeros((window.shape[0] - own - 2 * HALO, obs_dev), window.dtype)

    @pl.when(chan == 0)
    def _():
        window[:HALO, :] = rim

    @pl.when(chan == n_chan - 1)
    def _():
        window[own + HALO : own + 2 * HALO, :] = rim

    flip[...] = jnp.zeros_like(flip)
    wide[...] = jnp.zeros_like(wide)

    smalls[0].wait()
    smalls[1].wait()
    for place in range(3):
        load(place, 1).start()
    values = pred_in[...].astype(jnp.float32)
    first_row = 0
    for first in range(preds):
        count = preds - first
        wide[first_row : first_row + count, :] = values[first:, :] * values[first : first + 1, :]
        first_row += count
    wide[tall : tall + preds, :] = values

    def mask_line(line, carry):
        at = pl.ds(pl.multiple_of(line * slots, slots), slots)
        slot = lax.broadcasted_iota(jnp.int32, (tall + flat, slots), 1)
        live = jnp.where(slot < counts_in[line], wide[:, at], 0.0).astype(jnp.bfloat16)
        pairs_t[line] = live[:tall, :]
        preds_t[line] = live[tall:, :]
        return carry

    lax.fori_loop(0, lines, mask_line, 0, unroll=4)

    for copy in strips + smalls[2:]:
        copy.wait()
    for part in range(2):
        for place in range(3, 5):
            load(place, part).start()

    @pl.when(chan == 0)
    def _():
        ids_in[:, 0:LANES] = jnp.full((1, LANES), -1, jnp.int32)

    @pl.when(chan == n_chan - 1)
    def _():
        ids_in[:, LANES + own :] = jnp.full((1, LANES), -1, jnp.int32)

    def turn_band(block):
        for part in range(2):
            first = pl.multiple_of(block * WIDTH + part * TILE, TILE)
            own_ids = ids_in[:, pl.ds(first + TILE, TILE)].astype(jnp.float32)
            flip[part, 0:offsets, :] = inv_in[:, pl.ds(first, TILE)].astype(jnp.float32)
            flip[part, 64:65, :] = own_ids
            spun[part] = flip[part].T

    def skew_band(block, side):
        for part in range(2):
            first = pl.multiple_of(block * WIDTH + part * TILE, TILE)
            near = ids_in[:, pl.ds(first, 3 * TILE)].astype(jnp.float32)
            turned = spun[part]
            own_id = turned[:, 64:65]
            place = lax.broadcasted_iota(jnp.int32, turned.shape, 1)
            turned = jnp.where(place < offsets, turned, 0.0)
            skewed = pltpu.roll(
                jnp.concatenate([turned, jnp.zeros_like(turned)], axis=1),
                HALO - half,
                1,
                stride=1,
                stride_axis=0,
            )
            same = near[:, TILE - HALO : 3 * TILE - HALO] == own_id
            band = jnp.where(same, skewed, 0.0).astype(jnp.bfloat16)
            bands[side, part, 0] = band[:, :LANES]
            bands[side, part, 1] = band[:, LANES:]

    def wide_of(ref, first, second):
        return jnp.concatenate([ref[first, second, 0], ref[first, second, 1]], axis=1)

    def paired(ref, at):
        return jnp.concatenate([ref[at // LANES], ref[at // LANES + 1]], axis=1)

    def send_x(level):
        return pltpu.make_async_remote_copy(
            src_ref=x_code.at[level],
            dst_ref=landed_x.at[level],
            send_sem=x_send.at[level],
            recv_sem=x_recv.at[level],
            device_id=peer("obs", partner),
            device_id_type=MESH,
        )

    def send_z(level):
        return pltpu.make_async_remote_copy(
            src_ref=z_code.at[level],
            dst_ref=landed_z.at[lev],
            send_sem=z_send.at[level],
            recv_sem=z_recv.at[lev],
            device_id=peer("obs", 2 * level + col),
            device_id_type=MESH,
        )

    def from_z(level):
        return pltpu.make_async_remote_copy(
            src_ref=z_code.at[0],
            dst_ref=landed_z.at[level],
            send_sem=z_send.at[0],
            recv_sem=z_recv.at[level],
            device_id=peer("obs", 2 * level + col),
            device_id_type=MESH,
        )

    def send_straight(block):
        return pltpu.make_async_remote_copy(
            src_ref=d_code.at[block],
            dst_ref=landed_d.at[me],
            send_sem=d_send.at[block],
            recv_sem=d_recv.at[me],
            device_id=peer("obs", block),
            device_id_type=MESH,
        )

    def from_straight(source):
        return pltpu.make_async_remote_copy(
            src_ref=d_code.at[0],
            dst_ref=landed_d.at[source],
            send_sem=d_send.at[0],
            recv_sem=d_recv.at[source],
            device_id=peer("obs", source),
            device_id_type=MESH,
        )

    def encode(sums):
        gram = sums[:pad]
        rhs = sums[pad:]

        def grade(part):
            most = jnp.max(jnp.abs(part), axis=0, keepdims=True)
            return jnp.ceil(jnp.log2(jnp.maximum(most, 1e-30)))

        gram_grade = grade(gram)
        rhs_grade = grade(rhs)
        row = lax.broadcasted_iota(jnp.int32, rhs.shape, 0)
        gram = gram * (jnp.exp2(-gram_grade) * CODE)
        rhs = rhs * (jnp.exp2(-rhs_grade) * CODE)
        rhs = jnp.where(row == preds, gram_grade, rhs)
        rhs = jnp.where(row == preds + 1, rhs_grade, rhs)
        return jnp.round(jnp.concatenate([gram, rhs], axis=0)).astype(jnp.int32).astype(jnp.int16)

    def decode(code):
        values = code.astype(jnp.int32).astype(jnp.float32)
        gram_scale = jnp.exp2(values[pad + preds : pad + preds + 1]) * (1.0 / CODE)
        rhs_scale = jnp.exp2(values[pad + preds + 1 : pad + preds + 2]) * (1.0 / CODE)
        return jnp.concatenate([values[:pad] * gram_scale, values[pad:] * rhs_scale], axis=0)

    def accumulated(*accs):
        narrow = [[accs[4 * mxu + 2 * side : 4 * mxu + 2 * side + 2] for side in range(2)] for mxu in range(2)]
        tall_acc = [accs[8 + 2 * mxu : 10 + 2 * mxu] for mxu in range(2)]
        flat_acc = [accs[12 + 2 * mxu : 14 + 2 * mxu] for mxu in range(2)]

        def weigh(block, band, stage):
            start = pl.multiple_of(block * WIDTH, WIDTH)
            for mxu in range(2):
                at = (2 * stage + mxu) * OBS_TILE
                for part in range(2):
                    first = pl.multiple_of(start + part * TILE, TILE)
                    pltpu.matmul_push_rhs(
                        window[pl.ds(first, 2 * TILE), at : at + OBS_TILE],
                        staging_register=part,
                        mxu_index=mxu,
                    )
                    pltpu.matmul_acc_lhs(
                        narrow[mxu][stage % 2][part],
                        wide_of(bands, band, part),
                        load_staged_rhs=part,
                    )

        def turn_over(stage):
            for mxu in range(2):
                for part in range(2):
                    weighted = pltpu.matmul_pop(narrow[mxu][stage % 2][part])
                    turned_w[stage % 4, mxu, part] = weighted.astype(jnp.bfloat16).T

        def gather(side, stage):
            edge = jnp.bfloat16(huber_edge)
            for mxu in range(2):
                at = (2 * stage + mxu) * OBS_TILE
                weighted = wide_of(turned_w, stage % 4, mxu)
                qc_weight = edge / jnp.maximum(jnp.abs(weighted), edge)
                scaled = jnp.clip(weighted, -edge, edge)
                pltpu.matmul_push_rhs(qc_weight, staging_register=0, mxu_index=mxu)
                pltpu.matmul_acc_lhs(
                    tall_acc[mxu][side], paired(pairs_t, at), load_staged_rhs=0
                )
                pltpu.matmul_push_rhs(scaled, staging_register=1, mxu_index=mxu)
                pltpu.matmul_acc_lhs(
                    flat_acc[mxu][side], paired(preds_t, at), load_staged_rhs=1
                )

        def result(side):
            gram = pltpu.matmul_pop(tall_acc[0][side]) + pltpu.matmul_pop(tall_acc[1][side])
            rhs = pltpu.matmul_pop(flat_acc[0][side]) + pltpu.matmul_pop(flat_acc[1][side])
            return jnp.concatenate([gram[:pad], rhs], axis=0)

        def keep(step, sums):
            start = pl.multiple_of(block_at(step) * WIDTH, WIDTH)
            part_out[:, pl.ds(start, WIDTH)] = sums

        def joined(step, sums):
            level = level_at(turn_along(step))
            send_x(level).wait_recv()
            return sums + decode(landed_x[level])

        def pass_along(step, sums):
            level = level_at(turn_along(step))
            z_code[level] = encode(joined(step, sums))
            send_z(level).start()

        def deliver(step, sums):
            block = block_at(step)
            own_block = jnp.logical_and(early, block == col)

            @pl.when(jnp.logical_and(straight(step), own_block))
            def _():
                mine[...] = sums

            @pl.when(jnp.logical_and(straight(step), jnp.logical_not(own_block)))
            def _():
                d_code[block] = encode(sums)
                send_straight(block).start()

            @pl.when(across(step))
            def _():
                level = level_across(step)
                x_code[level] = encode(sums)
                send_x(level).start()

            @pl.when(jnp.logical_not(jnp.logical_or(straight(step), across(step))))
            def _():
                pass_along(step, sums)

        for acc in accs:
            pltpu.matmul_pop(acc)
        turn_band(block_at(0))
        skew_band(block_at(0), 0)
        pl.when(jnp.logical_not(early))(meet)
        for part in range(2):
            for place in range(5, blocks):
                load(place, part).start()
        turned_w[2:] = jnp.zeros((2,) + turned_w.shape[1:], turned_w.dtype)
        for place in range(3):
            load(place, 0).wait()
        def half_step(block, side, half_at):
            for stage in (2 * half_at, 2 * half_at + 1):
                weigh(block, side, stage)
            for stage in (2 * half_at, 2 * half_at + 1):
                if half_at == 0:
                    gather(1 - side, stages - 2 + stage)
                else:
                    gather(side, stage - 2)
            for stage in (2 * half_at, 2 * half_at + 1):
                turn_over(stage)

        def one_turn(turn, carry):
            for side in range(2):
                step = 2 * turn + side
                block = block_at(step)
                following = block_at(jnp.minimum(step + 1, blocks - 1))
                more = step + 1 < blocks
                turn_band(following)
                half_step(block, side, 0)
                sums = result(1 - side)
                due = [(place, 1) for place in range(3)] + [(3, 0), (4, 0)]
                if side == 1:
                    due = [(3, 1), (4, 1)]
                    due += [(place, part) for part in range(2) for place in range(5, blocks)]

                @pl.when(turn == 0)
                def _():
                    for place, part in due:
                        load(place, part).wait()

                if side == 1:
                    pl.when(jnp.logical_and(early, turn == 0))(meet)

                @pl.when(step > 0)
                def _():
                    if scatter:
                        deliver(step - 1, sums)
                    else:
                        keep(step - 1, sums)

                @pl.when(jnp.logical_and(more, jnp.logical_and(following == 0, chan > 0)))
                def _():
                    to_right.wait_recv()

                @pl.when(
                    jnp.logical_and(
                        more,
                        jnp.logical_and(following == blocks - 1, chan < n_chan - 1),
                    )
                )
                def _():
                    to_left.wait_recv()

                for half_at in range(1, stages // 2):
                    half_step(block, side, half_at)
                skew_band(following, 1 - side)
            return carry

        lax.fori_loop(0, levels, one_turn, 0)
        for stage in range(stages - 2, stages):
            gather(1, stage)
        sums = result(1)
        pl.when(chan > 0)(to_left.wait_send)
        pl.when(chan < n_chan - 1)(to_right.wait_send)
        if not scatter:
            keep(blocks - 1, sums)
            return

        def finish(sums):
            part_out[...] = sums * (1.0 / float(obs_dev * n_obs))

        @pl.when(early)
        def _():
            deliver(blocks - 1, sums)
            whole = mine[...]
            for away in range(1, n_obs):
                source = lax.rem(me + away, n_obs)
                from_straight(source).wait_recv()
                whole = whole + decode(landed_d[source])
            finish(whole)
            for away in range(1, n_obs):
                send_straight(lax.rem(me + away, n_obs)).wait_send()

        @pl.when(jnp.logical_not(early))
        def _():
            whole = joined(blocks - 1, sums)
            for source in range(2):
                from_straight(source).wait_recv()
                whole = whole + decode(landed_d[source])
            for turn in range(levels - 2):
                level = level_at(turn)
                from_z(level).wait_recv()
                whole = whole + decode(landed_z[level])
            finish(whole)
            for block in range(2):
                send_straight(block).wait_send()
            for turn in range(levels - 2):
                send_z(level_at(turn)).wait_send()
            for level in range(1, levels):
                send_x(level).wait_send()

    pl.run_scoped(accumulated, *acc_list(tall, flat))


def spread(preds, pad, part, gram_out, rhs_out, gram, rhs, sems):
    rhs[...] = part[pad : pad + preds, :]
    rhs_copy = pltpu.make_async_copy(rhs, rhs_out, sems.at[0])
    rhs_copy.start()
    for row, source in enumerate(mirror_rows(preds)):
        gram[row : row + 1, :] = part[source : source + 1, :]
    gram_copy = pltpu.make_async_copy(gram, gram_out, sems.at[1])
    gram_copy.start()
    rhs_copy.wait()
    gram_copy.wait()


def acc_list(tall, flat):
    specs = []
    for rows, copies in ((TILE, 4), (tall, 2), (flat, 2)):
        for mxu in range(2):
            specs += [pltpu.ACC(mxu)((rows, OBS_TILE), jnp.float32)] * copies
    return specs


def on_device(departures, predictors, inv_band, band_id, line_counts):
    own, obs_dev = departures.shape
    preds = predictors.shape[0]
    upper = preds * (preds + 1) // 2
    n_obs = lax.axis_size("obs")
    n_chan = lax.axis_size("chan")
    share = own // n_obs
    blocks = own // WIDTH
    scatter = share == WIDTH and n_obs == 8
    pad = padded(upper, 8)
    tall = padded(upper, 16)
    flat = padded(preds + 2, 16)
    rows = pad + flat
    if scatter:
        out_shape = (pltpu.VMEM((rows, share), jnp.float32),)
    else:
        out_shape = (jax.ShapeDtypeStruct((rows, own), jnp.float32),)
    vmem = pl.BlockSpec(memory_space=pltpu.VMEM)
    hbm = pl.BlockSpec(memory_space=pltpu.HBM)
    levels = blocks // 2
    kept = (levels, rows, WIDTH) if scatter else (1, 8, LANES)
    many = (n_obs,) + kept[1:] if scatter else kept
    dma = pltpu.SemaphoreType.DMA
    outs = pl.pallas_call(
        functools.partial(kernel, n_obs, n_chan, scatter),
        out_shape=out_shape,
        in_specs=[hbm] * 5,
        out_specs=tuple(vmem for _ in out_shape),
        scratch_shapes=[
            pltpu.VMEM((own + 4 * HALO, obs_dev), jnp.bfloat16),
            pltpu.VMEM((2, HALO, obs_dev), jnp.bfloat16),
            pltpu.VMEM(predictors.shape, jnp.bfloat16),
            pltpu.VMEM(inv_band.shape, jnp.bfloat16),
            pltpu.VMEM((1, own + 2 * LANES), jnp.int32),
            pltpu.SMEM(line_counts.shape, jnp.int32),
            pltpu.VMEM((tall + flat, obs_dev), jnp.float32),
            pltpu.VMEM((obs_dev // LANES, tall, LANES), jnp.bfloat16),
            pltpu.VMEM((obs_dev // LANES, flat, LANES), jnp.bfloat16),
            pltpu.VMEM((2, LANES, TILE), jnp.float32),
            pltpu.VMEM((2, TILE, LANES), jnp.float32),
            pltpu.VMEM((2, 2, 2, TILE, LANES), jnp.bfloat16),
            pltpu.VMEM((4, 2, 2, OBS_TILE, LANES), jnp.bfloat16),
            pltpu.VMEM((rows, WIDTH), jnp.float32),
            pltpu.VMEM(kept, jnp.int16),
            pltpu.VMEM(kept, jnp.int16),
            pltpu.VMEM(many, jnp.int16),
            pltpu.VMEM(kept, jnp.int16),
            pltpu.VMEM(kept, jnp.int16),
            pltpu.VMEM(many, jnp.int16),
            dma((8,)),
            dma((2, blocks)),
            dma((2,)),
            dma((2,)),
            dma((levels,)),
            dma((levels,)),
            dma((levels,)),
            dma((levels,)),
            dma((n_obs,)),
            dma((n_obs,)),
        ],
        compiler_params=pltpu.CompilerParams(
            collective_id=0,
            has_side_effects=True,
            vmem_limit_bytes=67043328 - 120 * 1024,
        ),
        name="normal_equations",
    )(departures, predictors, inv_band, band_id[None, :], line_counts)
    if scatter:
        return pl.pallas_call(
            functools.partial(spread, preds, pad),
            out_shape=(
                jax.ShapeDtypeStruct((preds * preds, share), jnp.float32),
                jax.ShapeDtypeStruct((preds, share), jnp.float32),
            ),
            in_specs=[vmem],
            out_specs=(hbm, hbm),
            scratch_shapes=[
                pltpu.VMEM((preds * preds, share), jnp.float32),
                pltpu.VMEM((preds, share), jnp.float32),
                dma((2,)),
            ],
            compiler_params=pltpu.CompilerParams(vmem_limit_bytes=1024 * 1024),
            name="mirror",
        )(outs[0])
    factor = 1.0 / float(obs_dev * n_obs)
    part = lax.psum_scatter(outs[0], "obs", scatter_dimension=1, tiled=True) * factor
    mirror = np.array(mirror_rows(preds))
    return part[mirror], part[pad : pad + preds]


def solution(mesh):
    in_specs = (P("chan", "obs"), P(None, "obs"), P(None, "chan"), P(), P("obs"))
    out_specs = (P(None, ("chan", "obs")), P(None, ("chan", "obs")))
    return jax.shard_map(
        on_device, mesh=mesh, in_specs=in_specs, out_specs=out_specs, check_vma=False
    )
```

```python
import functools

import jax
import jax.numpy as jnp
import numpy as np
from jax import lax
from jax.experimental import pallas as pl
from jax.experimental.pallas import tpu as pltpu
from jax.sharding import PartitionSpec as P

huber_edge = 1.0
LANES = 128
HALO = 32
TILE = 128
WIDTH = 2 * TILE
OBS_TILE = 256
CODE = 32512.0
MESH = pl.DeviceIdType.MESH


def mirror_rows(count):
    rows = []
    for first in range(count):
        for second in range(count):
            low = min(first, second)
            high = max(first, second)
            rows.append(low * count - low * (low - 1) // 2 + high - low)
    return rows


def padded(count, unit):
    return -(-count // unit) * unit


def peer(axis, index):
    if axis == "obs":
        return (index, lax.axis_index("chan"))
    return (lax.axis_index("obs"), index)


def kernel(n_obs, n_chan, scatter, dep, pred, inv, ids, counts, *rest):
    part_out = rest[0]
    rest = rest[1:]
    (
        window,
        strip,
        pred_in,
        inv_in,
        ids_in,
        counts_in,
        wide,
        pairs_t,
        preds_t,
        flip,
        spun,
        bands,
        turned_w,
        mine,
        x_code,
        z_code,
        d_code,
        landed_x,
        landed_z,
        landed_d,
        small_sem,
        load_sem,
        halo_send,
        halo_recv,
        x_send,
        x_recv,
        z_send,
        z_recv,
        d_send,
        d_recv,
    ) = rest
    own, obs_dev = dep.shape
    preds = pred.shape[0]
    offsets = inv.shape[0]
    half = offsets // 2
    upper = preds * (preds + 1) // 2
    pad = padded(upper, 8)
    tall = pairs_t.shape[1]
    flat = preds_t.shape[1]
    blocks = own // WIDTH
    levels = blocks // 2
    stages = obs_dev // (2 * OBS_TILE)
    lines = counts.shape[0]
    slots = obs_dev // lines
    me = lax.axis_index("obs")
    chan = lax.axis_index("chan")
    right = lax.rem(chan + 1, n_chan)
    left = lax.rem(chan + n_chan - 1, n_chan)
    if scatter:
        col = lax.rem(me, 2)
        lev = lax.div(me, 2)
        partner = me + 1 - 2 * col
    else:
        col = 1
        lev = levels - 1
        partner = me
    early = lev == 0 if scatter else me < 0

    def is_any(step, choices):
        found = step == choices[0]
        for choice in choices[1:]:
            found = jnp.logical_or(found, step == choice)
        return found

    def straight(step):
        return jnp.logical_or(early, is_any(step, (0, 2)))

    def across(step):
        return jnp.logical_and(jnp.logical_not(early), is_any(step, (1, 3, 4)))

    def level_at(turn):
        shifted = jnp.where(turn + 1 >= lev, turn + 2, turn + 1)
        return jnp.where(turn == levels - 2, lev, shifted)

    def level_across(step):
        return level_at(jnp.where(step < 2, 0, step - 2))

    def turn_along(step):
        return step - 5

    def block_at(step):
        step = jnp.int32(step)
        if not scatter:
            return jnp.where(step < 2, 1 - step, step)
        odd_end = jnp.where(step < 6, step - 4, jnp.where(step == 6, 7, 2))
        even_end = jnp.where(step == 4, 2, jnp.where(step == 5, 7, 7 - step))
        ahead = jnp.where(step < 4, 6 - step, jnp.where(col == 1, odd_end, even_end))
        later = jnp.where(
            is_any(step, (0, 2)),
            jnp.where(step == 0, 1, 0),
            jnp.where(
                is_any(step, (1, 3, 4)),
                2 * level_across(step) + 1 - col,
                2 * level_at(turn_along(step)) + col,
            ),
        )
        return jnp.where(early, ahead, later)

    def chunk_at(place):
        if not scatter:
            return place
        aside = jnp.where(place == 6, 3, jnp.where(is_any(place, (3, 4, 5)), place + 1, place))
        later = jnp.where(jnp.logical_and(lev == 1, col == 0), aside, place)
        return jnp.where(early, jnp.where(place < 3, blocks - 3 + place, blocks - 1 - place), later)

    barrier = pltpu.get_barrier_semaphore()
    for index in (left, right):
        pl.semaphore_signal(barrier, inc=1, device_id=peer("chan", index), device_id_type=MESH)
    greeted = 2
    if scatter:
        pl.semaphore_signal(barrier, inc=1, device_id=peer("obs", partner), device_id_type=MESH)
        for away in range(1, levels):
            index = 2 * lax.rem(lev + away, levels) + col
            pl.semaphore_signal(barrier, inc=1, device_id=peer("obs", index), device_id_type=MESH)

        @pl.when(early)
        def _():
            for level in range(1, levels):
                index = 2 * level + 1 - col
                pl.semaphore_signal(
                    barrier, inc=1, device_id=peer("obs", index), device_id_type=MESH
                )

        @pl.when(jnp.logical_not(early))
        def _():
            pl.semaphore_signal(barrier, inc=1, device_id=peer("obs", 1 - col), device_id_type=MESH)

        greeted += levels + jnp.where(early, levels - 1, 1)

    base = pl.multiple_of(chan * own, own)
    smalls = [
        pltpu.make_async_copy(pred, pred_in, small_sem.at[0]),
        pltpu.make_async_copy(counts, counts_in, small_sem.at[1]),
        pltpu.make_async_copy(inv, inv_in, small_sem.at[2]),
        pltpu.make_async_copy(
            ids.at[:, pl.ds(base, own)], ids_in.at[:, pl.ds(LANES, own)], small_sem.at[3]
        ),
        pltpu.make_async_copy(
            ids.at[:, pl.ds(pl.multiple_of(jnp.maximum(base - LANES, 0), LANES), LANES)],
            ids_in.at[:, pl.ds(0, LANES)],
            small_sem.at[4],
        ),
        pltpu.make_async_copy(
            ids.at[
                :, pl.ds(pl.multiple_of(jnp.minimum(base + own, own * n_chan - LANES), LANES), LANES)
            ],
            ids_in.at[:, pl.ds(LANES + own, LANES)],
            small_sem.at[5],
        ),
    ]
    for copy in smalls[:2]:
        copy.start()

    fore = obs_dev // stages * 2

    def load(place, part):
        chunk = chunk_at(jnp.int32(place))
        start = pl.multiple_of(chunk * WIDTH, WIDTH)
        at = pl.ds(0, fore) if part == 0 else pl.ds(fore, obs_dev - fore)
        return pltpu.make_async_copy(
            dep.at[pl.ds(start, WIDTH), at],
            window.at[pl.ds(start + HALO, WIDTH), at],
            load_sem.at[part, place],
        )

    strips = [
        pltpu.make_async_copy(dep.at[pl.ds(0, HALO), :], strip.at[0], small_sem.at[6]),
        pltpu.make_async_copy(dep.at[pl.ds(own - HALO, HALO), :], strip.at[1], small_sem.at[7]),
    ]
    for copy in strips + smalls[2:]:
        copy.start()
    for place in range(3):
        load(place, 0).start()

    to_left = pltpu.make_async_remote_copy(
        src_ref=strip.at[0],
        dst_ref=window.at[pl.ds(own + HALO, HALO), :],
        send_sem=halo_send.at[0],
        recv_sem=halo_recv.at[0],
        device_id=peer("chan", left),
        device_id_type=MESH,
    )
    to_right = pltpu.make_async_remote_copy(
        src_ref=strip.at[1],
        dst_ref=window.at[pl.ds(0, HALO), :],
        send_sem=halo_send.at[1],
        recv_sem=halo_recv.at[1],
        device_id=peer("chan", right),
        device_id_type=MESH,
    )

    def meet():
        pl.semaphore_wait(barrier, greeted)
        pl.when(chan > 0)(to_left.start)
        pl.when(chan < n_chan - 1)(to_right.start)

    rim = jnp.zeros((HALO, obs_dev), window.dtype)
    window[own + 2 * HALO :, :] = jnp.zeros((window.shape[0] - own - 2 * HALO, obs_dev), window.dtype)

    @pl.when(chan == 0)
    def _():
        window[:HALO, :] = rim

    @pl.when(chan == n_chan - 1)
    def _():
        window[own + HALO : own + 2 * HALO, :] = rim

    flip[...] = jnp.zeros_like(flip)
    wide[...] = jnp.zeros_like(wide)

    smalls[0].wait()
    smalls[1].wait()
    for place in range(3):
        load(place, 1).start()
    values = pred_in[...].astype(jnp.float32)
    first_row = 0
    for first in range(preds):
        count = preds - first
        wide[first_row : first_row + count, :] = values[first:, :] * values[first : first + 1, :]
        first_row += count
    wide[tall : tall + preds, :] = values

    def mask_line(line, carry):
        at = pl.ds(pl.multiple_of(line * slots, slots), slots)
        slot = lax.broadcasted_iota(jnp.int32, (tall + flat, slots), 1)
        live = jnp.where(slot < counts_in[line], wide[:, at], 0.0).astype(jnp.bfloat16)
        pairs_t[line] = live[:tall, :]
        preds_t[line] = live[tall:, :]
        return carry

    lax.fori_loop(0, lines, mask_line, 0, unroll=4)

    for copy in strips + smalls[2:]:
        copy.wait()
    for part in range(2):
        for place in range(3, 5):
            load(place, part).start()

    @pl.when(chan == 0)
    def _():
        ids_in[:, 0:LANES] = jnp.full((1, LANES), -1, jnp.int32)

    @pl.when(chan == n_chan - 1)
    def _():
        ids_in[:, LANES + own :] = jnp.full((1, LANES), -1, jnp.int32)

    def turn_band(block):
        for part in range(2):
            first = pl.multiple_of(block * WIDTH + part * TILE, TILE)
            own_ids = ids_in[:, pl.ds(first + TILE, TILE)].astype(jnp.float32)
            flip[part, 0:offsets, :] = inv_in[:, pl.ds(first, TILE)].astype(jnp.float32)
            flip[part, 64:65, :] = own_ids
            spun[part] = flip[part].T

    def skew_band(block, side):
        for part in range(2):
            first = pl.multiple_of(block * WIDTH + part * TILE, TILE)
            near = ids_in[:, pl.ds(first, 3 * TILE)].astype(jnp.float32)
            turned = spun[part]
            own_id = turned[:, 64:65]
            place = lax.broadcasted_iota(jnp.int32, turned.shape, 1)
            turned = jnp.where(place < offsets, turned, 0.0)
            skewed = pltpu.roll(
                jnp.concatenate([turned, jnp.zeros_like(turned)], axis=1),
                HALO - half,
                1,
                stride=1,
                stride_axis=0,
            )
            same = near[:, TILE - HALO : 3 * TILE - HALO] == own_id
            band = jnp.where(same, skewed, 0.0).astype(jnp.bfloat16)
            bands[side, part, 0] = band[:, :LANES]
            bands[side, part, 1] = band[:, LANES:]

    def wide_of(ref, first, second):
        return jnp.concatenate([ref[first, second, 0], ref[first, second, 1]], axis=1)

    def paired(ref, at):
        return jnp.concatenate([ref[at // LANES], ref[at // LANES + 1]], axis=1)

    def send_x(level):
        return pltpu.make_async_remote_copy(
            src_ref=x_code.at[level],
            dst_ref=landed_x.at[level],
            send_sem=x_send.at[level],
            recv_sem=x_recv.at[level],
            device_id=peer("obs", partner),
            device_id_type=MESH,
        )

    def send_z(level):
        return pltpu.make_async_remote_copy(
            src_ref=z_code.at[level],
            dst_ref=landed_z.at[lev],
            send_sem=z_send.at[level],
            recv_sem=z_recv.at[lev],
            device_id=peer("obs", 2 * level + col),
            device_id_type=MESH,
        )

    def from_z(level):
        return pltpu.make_async_remote_copy(
            src_ref=z_code.at[0],
            dst_ref=landed_z.at[level],
            send_sem=z_send.at[0],
            recv_sem=z_recv.at[level],
            device_id=peer("obs", 2 * level + col),
            device_id_type=MESH,
        )

    def send_straight(block):
        return pltpu.make_async_remote_copy(
            src_ref=d_code.at[block],
            dst_ref=landed_d.at[me],
            send_sem=d_send.at[block],
            recv_sem=d_recv.at[me],
            device_id=peer("obs", block),
            device_id_type=MESH,
        )

    def from_straight(source):
        return pltpu.make_async_remote_copy(
            src_ref=d_code.at[0],
            dst_ref=landed_d.at[source],
            send_sem=d_send.at[0],
            recv_sem=d_recv.at[source],
            device_id=peer("obs", source),
            device_id_type=MESH,
        )

    def encode(sums):
        gram = sums[:pad]
        rhs = sums[pad:]

        def grade(part):
            most = jnp.max(jnp.abs(part), axis=0, keepdims=True)
            return jnp.ceil(jnp.log2(jnp.maximum(most, 1e-30)))

        gram_grade = grade(gram)
        rhs_grade = grade(rhs)
        row = lax.broadcasted_iota(jnp.int32, rhs.shape, 0)
        gram = gram * (jnp.exp2(-gram_grade) * CODE)
        rhs = rhs * (jnp.exp2(-rhs_grade) * CODE)
        rhs = jnp.where(row == preds, gram_grade, rhs)
        rhs = jnp.where(row == preds + 1, rhs_grade, rhs)
        return jnp.round(jnp.concatenate([gram, rhs], axis=0)).astype(jnp.int32).astype(jnp.int16)

    def decode(code):
        values = code.astype(jnp.int32).astype(jnp.float32)
        gram_scale = jnp.exp2(values[pad + preds : pad + preds + 1]) * (1.0 / CODE)
        rhs_scale = jnp.exp2(values[pad + preds + 1 : pad + preds + 2]) * (1.0 / CODE)
        return jnp.concatenate([values[:pad] * gram_scale, values[pad:] * rhs_scale], axis=0)

    def accumulated(*accs):
        narrow = [[accs[4 * mxu + 2 * side : 4 * mxu + 2 * side + 2] for side in range(2)] for mxu in range(2)]
        tall_acc = [accs[8 + 2 * mxu : 10 + 2 * mxu] for mxu in range(2)]
        flat_acc = [accs[12 + 2 * mxu : 14 + 2 * mxu] for mxu in range(2)]

        def weigh(block, band, stage):
            start = pl.multiple_of(block * WIDTH, WIDTH)
            for mxu in range(2):
                at = (2 * stage + mxu) * OBS_TILE
                for part in range(2):
                    first = pl.multiple_of(start + part * TILE, TILE)
                    pltpu.matmul_push_rhs(
                        window[pl.ds(first, 2 * TILE), at : at + OBS_TILE],
                        staging_register=part,
                        mxu_index=mxu,
                    )
                    pltpu.matmul_acc_lhs(
                        narrow[mxu][stage % 2][part],
                        wide_of(bands, band, part),
                        load_staged_rhs=part,
                    )

        def turn_over(stage):
            for mxu in range(2):
                for part in range(2):
                    weighted = pltpu.matmul_pop(narrow[mxu][stage % 2][part])
                    turned_w[stage % 4, mxu, part] = weighted.astype(jnp.bfloat16).T

        def gather(side, stage):
            edge = jnp.bfloat16(huber_edge)
            for mxu in range(2):
                at = (2 * stage + mxu) * OBS_TILE
                weighted = wide_of(turned_w, stage % 4, mxu)
                qc_weight = edge / jnp.maximum(jnp.abs(weighted), edge)
                scaled = jnp.clip(weighted, -edge, edge)
                pltpu.matmul_push_rhs(qc_weight, staging_register=0, mxu_index=mxu)
                pltpu.matmul_acc_lhs(
                    tall_acc[mxu][side], paired(pairs_t, at), load_staged_rhs=0
                )
                pltpu.matmul_push_rhs(scaled, staging_register=1, mxu_index=mxu)
                pltpu.matmul_acc_lhs(
                    flat_acc[mxu][side], paired(preds_t, at), load_staged_rhs=1
                )

        def result(side):
            gram = pltpu.matmul_pop(tall_acc[0][side]) + pltpu.matmul_pop(tall_acc[1][side])
            rhs = pltpu.matmul_pop(flat_acc[0][side]) + pltpu.matmul_pop(flat_acc[1][side])
            return jnp.concatenate([gram[:pad], rhs], axis=0)

        def keep(step, sums):
            start = pl.multiple_of(block_at(step) * WIDTH, WIDTH)
            part_out[:, pl.ds(start, WIDTH)] = sums

        def joined(step, sums):
            level = level_at(turn_along(step))
            send_x(level).wait_recv()
            return sums + decode(landed_x[level])

        def pass_along(step, sums):
            level = level_at(turn_along(step))
            z_code[level] = encode(joined(step, sums))
            send_z(level).start()

        def deliver(step, sums):
            block = block_at(step)
            own_block = jnp.logical_and(early, block == col)

            @pl.when(jnp.logical_and(straight(step), own_block))
            def _():
                mine[...] = sums

            @pl.when(jnp.logical_and(straight(step), jnp.logical_not(own_block)))
            def _():
                d_code[block] = encode(sums)
                send_straight(block).start()

            @pl.when(across(step))
            def _():
                level = level_across(step)
                x_code[level] = encode(sums)
                send_x(level).start()

            @pl.when(jnp.logical_not(jnp.logical_or(straight(step), across(step))))
            def _():
                pass_along(step, sums)

        for acc in accs:
            pltpu.matmul_pop(acc)
        turn_band(block_at(0))
        skew_band(block_at(0), 0)
        pl.when(jnp.logical_not(early))(meet)
        for part in range(2):
            for place in range(5, blocks):
                load(place, part).start()
        turned_w[2:] = jnp.zeros((2,) + turned_w.shape[1:], turned_w.dtype)
        for place in range(3):
            load(place, 0).wait()
        def half_step(block, side, half_at):
            for stage in (2 * half_at, 2 * half_at + 1):
                weigh(block, side, stage)
            for stage in (2 * half_at, 2 * half_at + 1):
                if half_at == 0:
                    gather(1 - side, stages - 2 + stage)
                else:
                    gather(side, stage - 2)
            for stage in (2 * half_at, 2 * half_at + 1):
                turn_over(stage)

        def one_turn(turn, carry):
            for side in range(2):
                step = 2 * turn + side
                block = block_at(step)
                following = block_at(jnp.minimum(step + 1, blocks - 1))
                more = step + 1 < blocks
                turn_band(following)
                half_step(block, side, 0)
                sums = result(1 - side)
                due = [(place, 1) for place in range(3)] + [(3, 0), (4, 0)]
                if side == 1:
                    due = [(3, 1), (4, 1)]
                    due += [(place, part) for part in range(2) for place in range(6 - part, blocks)]

                @pl.when(turn == 0)
                def _():
                    for place, part in due:
                        load(place, part).wait()
                    pl.when((lev == 1) == (side == 0))(load(5, 0).wait)

                if side == 1:
                    pl.when(jnp.logical_and(early, turn == 0))(meet)

                @pl.when(step > 0)
                def _():
                    if scatter:
                        deliver(step - 1, sums)
                    else:
                        keep(step - 1, sums)

                @pl.when(jnp.logical_and(more, jnp.logical_and(following == 0, chan > 0)))
                def _():
                    to_right.wait_recv()

                @pl.when(
                    jnp.logical_and(
                        more,
                        jnp.logical_and(following == blocks - 1, chan < n_chan - 1),
                    )
                )
                def _():
                    to_left.wait_recv()

                for half_at in range(1, stages // 2):
                    half_step(block, side, half_at)
                skew_band(following, 1 - side)
            return carry

        lax.fori_loop(0, levels, one_turn, 0)
        for stage in range(stages - 2, stages):
            gather(1, stage)
        sums = result(1)
        pl.when(chan > 0)(to_left.wait_send)
        pl.when(chan < n_chan - 1)(to_right.wait_send)
        if not scatter:
            keep(blocks - 1, sums)
            return

        def finish(sums):
            part_out[...] = sums * (1.0 / float(obs_dev * n_obs))

        @pl.when(early)
        def _():
            deliver(blocks - 1, sums)
            whole = mine[...]
            for away in range(1, n_obs):
                source = lax.rem(me + away, n_obs)
                from_straight(source).wait_recv()
                whole = whole + decode(landed_d[source])
            finish(whole)
            for away in range(1, n_obs):
                send_straight(lax.rem(me + away, n_obs)).wait_send()

        @pl.when(jnp.logical_not(early))
        def _():
            whole = joined(blocks - 1, sums)
            for source in range(2):
                from_straight(source).wait_recv()
                whole = whole + decode(landed_d[source])
            for turn in range(levels - 2):
                level = level_at(turn)
                from_z(level).wait_recv()
                whole = whole + decode(landed_z[level])
            finish(whole)
            for block in range(2):
                send_straight(block).wait_send()
            for turn in range(levels - 2):
                send_z(level_at(turn)).wait_send()
            for level in range(1, levels):
                send_x(level).wait_send()

    pl.run_scoped(accumulated, *acc_list(tall, flat))


def spread(preds, pad, part, gram_out, rhs_out, gram, rhs, sems):
    rhs[...] = part[pad : pad + preds, :]
    rhs_copy = pltpu.make_async_copy(rhs, rhs_out, sems.at[0])
    rhs_copy.start()
    for row, source in enumerate(mirror_rows(preds)):
        gram[row : row + 1, :] = part[source : source + 1, :]
    gram_copy = pltpu.make_async_copy(gram, gram_out, sems.at[1])
    gram_copy.start()
    rhs_copy.wait()
    gram_copy.wait()


def acc_list(tall, flat):
    specs = []
    for rows, copies in ((TILE, 4), (tall, 2), (flat, 2)):
        for mxu in range(2):
            specs += [pltpu.ACC(mxu)((rows, OBS_TILE), jnp.float32)] * copies
    return specs


def on_device(departures, predictors, inv_band, band_id, line_counts):
    own, obs_dev = departures.shape
    preds = predictors.shape[0]
    upper = preds * (preds + 1) // 2
    n_obs = lax.axis_size("obs")
    n_chan = lax.axis_size("chan")
    share = own // n_obs
    blocks = own // WIDTH
    scatter = share == WIDTH and n_obs == 8
    pad = padded(upper, 8)
    tall = padded(upper, 16)
    flat = padded(preds + 2, 16)
    rows = pad + flat
    if scatter:
        out_shape = (pltpu.VMEM((rows, share), jnp.float32),)
    else:
        out_shape = (jax.ShapeDtypeStruct((rows, own), jnp.float32),)
    vmem = pl.BlockSpec(memory_space=pltpu.VMEM)
    hbm = pl.BlockSpec(memory_space=pltpu.HBM)
    levels = blocks // 2
    kept = (levels, rows, WIDTH) if scatter else (1, 8, LANES)
    many = (n_obs,) + kept[1:] if scatter else kept
    dma = pltpu.SemaphoreType.DMA
    outs = pl.pallas_call(
        functools.partial(kernel, n_obs, n_chan, scatter),
        out_shape=out_shape,
        in_specs=[hbm] * 5,
        out_specs=tuple(vmem for _ in out_shape),
        scratch_shapes=[
            pltpu.VMEM((own + 4 * HALO, obs_dev), jnp.bfloat16),
            pltpu.VMEM((2, HALO, obs_dev), jnp.bfloat16),
            pltpu.VMEM(predictors.shape, jnp.bfloat16),
            pltpu.VMEM(inv_band.shape, jnp.bfloat16),
            pltpu.VMEM((1, own + 2 * LANES), jnp.int32),
            pltpu.SMEM(line_counts.shape, jnp.int32),
            pltpu.VMEM((tall + flat, obs_dev), jnp.float32),
            pltpu.VMEM((obs_dev // LANES, tall, LANES), jnp.bfloat16),
            pltpu.VMEM((obs_dev // LANES, flat, LANES), jnp.bfloat16),
            pltpu.VMEM((2, LANES, TILE), jnp.float32),
            pltpu.VMEM((2, TILE, LANES), jnp.float32),
            pltpu.VMEM((2, 2, 2, TILE, LANES), jnp.bfloat16),
            pltpu.VMEM((4, 2, 2, OBS_TILE, LANES), jnp.bfloat16),
            pltpu.VMEM((rows, WIDTH), jnp.float32),
            pltpu.VMEM(kept, jnp.int16),
            pltpu.VMEM(kept, jnp.int16),
            pltpu.VMEM(many, jnp.int16),
            pltpu.VMEM(kept, jnp.int16),
            pltpu.VMEM(kept, jnp.int16),
            pltpu.VMEM(many, jnp.int16),
            dma((8,)),
            dma((2, blocks)),
            dma((2,)),
            dma((2,)),
            dma((levels,)),
            dma((levels,)),
            dma((levels,)),
            dma((levels,)),
            dma((n_obs,)),
            dma((n_obs,)),
        ],
        compiler_params=pltpu.CompilerParams(
            collective_id=0,
            has_side_effects=True,
            vmem_limit_bytes=67043328 - 120 * 1024,
        ),
        name="normal_equations",
    )(departures, predictors, inv_band, band_id[None, :], line_counts)
    if scatter:
        return pl.pallas_call(
            functools.partial(spread, preds, pad),
            out_shape=(
                jax.ShapeDtypeStruct((preds * preds, share), jnp.float32),
                jax.ShapeDtypeStruct((preds, share), jnp.float32),
            ),
            in_specs=[vmem],
            out_specs=(hbm, hbm),
            scratch_shapes=[
                pltpu.VMEM((preds * preds, share), jnp.float32),
                pltpu.VMEM((preds, share), jnp.float32),
                dma((2,)),
            ],
            compiler_params=pltpu.CompilerParams(vmem_limit_bytes=1024 * 1024),
            name="mirror",
        )(outs[0])
    factor = 1.0 / float(obs_dev * n_obs)
    part = lax.psum_scatter(outs[0], "obs", scatter_dimension=1, tiled=True) * factor
    mirror = np.array(mirror_rows(preds))
    return part[mirror], part[pad : pad + preds]


def solution(mesh):
    in_specs = (P("chan", "obs"), P(None, "obs"), P(None, "chan"), P(), P("obs"))
    out_specs = (P(None, ("chan", "obs")), P(None, ("chan", "obs")))
    return jax.shard_map(
        on_device, mesh=mesh, in_specs=in_specs, out_specs=out_specs, check_vma=False
    )
```

```python
import functools

import jax
import jax.numpy as jnp
import numpy as np
from jax import lax
from jax.experimental import pallas as pl
from jax.experimental.pallas import tpu as pltpu
from jax.sharding import PartitionSpec as P

huber_edge = 1.0
LANES = 128
HALO = 32
TILE = 128
WIDTH = 2 * TILE
OBS_TILE = 256
CODE = 32512.0
MESH = pl.DeviceIdType.MESH


def mirror_rows(count):
    rows = []
    for first in range(count):
        for second in range(count):
            low = min(first, second)
            high = max(first, second)
            rows.append(low * count - low * (low - 1) // 2 + high - low)
    return rows


def padded(count, unit):
    return -(-count // unit) * unit


def peer(axis, index):
    if axis == "obs":
        return (index, lax.axis_index("chan"))
    return (lax.axis_index("obs"), index)


def kernel(n_obs, n_chan, scatter, dep, pred, inv, ids, counts, *rest):
    part_out = rest[0]
    rest = rest[1:]
    (
        window,
        strip,
        pred_in,
        inv_in,
        ids_in,
        counts_in,
        wide,
        pairs_t,
        preds_t,
        flip,
        spun,
        bands,
        turned_w,
        mine,
        x_code,
        z_code,
        d_code,
        landed_x,
        landed_z,
        landed_d,
        small_sem,
        load_sem,
        halo_send,
        halo_recv,
        x_send,
        x_recv,
        z_send,
        z_recv,
        d_send,
        d_recv,
    ) = rest
    own, obs_dev = dep.shape
    preds = pred.shape[0]
    offsets = inv.shape[0]
    half = offsets // 2
    upper = preds * (preds + 1) // 2
    pad = padded(upper, 8)
    tall = pairs_t.shape[1]
    flat = preds_t.shape[1]
    blocks = own // WIDTH
    levels = blocks // 2
    stages = obs_dev // (2 * OBS_TILE)
    lines = counts.shape[0]
    slots = obs_dev // lines
    me = lax.axis_index("obs")
    chan = lax.axis_index("chan")
    right = lax.rem(chan + 1, n_chan)
    left = lax.rem(chan + n_chan - 1, n_chan)
    if scatter:
        col = lax.rem(me, 2)
        lev = lax.div(me, 2)
        partner = me + 1 - 2 * col
    else:
        col = 1
        lev = levels - 1
        partner = me
    early = lev == 0 if scatter else me < 0

    def is_any(step, choices):
        found = step == choices[0]
        for choice in choices[1:]:
            found = jnp.logical_or(found, step == choice)
        return found

    def straight(step):
        return jnp.logical_or(early, is_any(step, (0, 2)))

    def across(step):
        return jnp.logical_and(jnp.logical_not(early), is_any(step, (1, 3, 4)))

    def level_at(turn):
        shifted = jnp.where(turn + 1 >= lev, turn + 2, turn + 1)
        return jnp.where(turn == levels - 2, lev, shifted)

    def level_across(step):
        return level_at(jnp.where(step < 2, 0, step - 2))

    def turn_along(step):
        return step - 5

    def block_at(step):
        step = jnp.int32(step)
        if not scatter:
            return jnp.where(step < 2, 1 - step, step)
        odd_end = jnp.where(step < 6, step - 4, jnp.where(step == 6, 7, 2))
        even_end = jnp.where(step == 4, 2, jnp.where(step == 5, 7, 7 - step))
        ahead = jnp.where(step < 4, 6 - step, jnp.where(col == 1, odd_end, even_end))
        later = jnp.where(
            is_any(step, (0, 2)),
            jnp.where(step == 0, 1, 0),
            jnp.where(
                is_any(step, (1, 3, 4)),
                2 * level_across(step) + 1 - col,
                2 * level_at(turn_along(step)) + col,
            ),
        )
        return jnp.where(early, ahead, later)

    def chunk_at(place):
        if not scatter:
            return place
        aside = jnp.where(place == 6, 3, jnp.where(is_any(place, (3, 4, 5)), place + 1, place))
        later = jnp.where(jnp.logical_and(lev == 1, col == 0), aside, place)
        return jnp.where(early, jnp.where(place < 3, blocks - 3 + place, blocks - 1 - place), later)

    barrier = pltpu.get_barrier_semaphore()
    for index in (left, right):
        pl.semaphore_signal(barrier, inc=1, device_id=peer("chan", index), device_id_type=MESH)
    greeted = 2
    if scatter:
        pl.semaphore_signal(barrier, inc=1, device_id=peer("obs", partner), device_id_type=MESH)
        for away in range(1, levels):
            index = 2 * lax.rem(lev + away, levels) + col
            pl.semaphore_signal(barrier, inc=1, device_id=peer("obs", index), device_id_type=MESH)

        @pl.when(early)
        def _():
            for level in range(1, levels):
                index = 2 * level + 1 - col
                pl.semaphore_signal(
                    barrier, inc=1, device_id=peer("obs", index), device_id_type=MESH
                )

        @pl.when(jnp.logical_not(early))
        def _():
            pl.semaphore_signal(barrier, inc=1, device_id=peer("obs", 1 - col), device_id_type=MESH)

        greeted += levels + jnp.where(early, levels - 1, 1)

    base = pl.multiple_of(chan * own, own)
    smalls = [
        pltpu.make_async_copy(pred, pred_in, small_sem.at[0]),
        pltpu.make_async_copy(counts, counts_in, small_sem.at[1]),
        pltpu.make_async_copy(inv, inv_in, small_sem.at[2]),
        pltpu.make_async_copy(
            ids.at[:, pl.ds(base, own)], ids_in.at[:, pl.ds(LANES, own)], small_sem.at[3]
        ),
        pltpu.make_async_copy(
            ids.at[:, pl.ds(pl.multiple_of(jnp.maximum(base - LANES, 0), LANES), LANES)],
            ids_in.at[:, pl.ds(0, LANES)],
            small_sem.at[4],
        ),
        pltpu.make_async_copy(
            ids.at[
                :, pl.ds(pl.multiple_of(jnp.minimum(base + own, own * n_chan - LANES), LANES), LANES)
            ],
            ids_in.at[:, pl.ds(LANES + own, LANES)],
            small_sem.at[5],
        ),
    ]
    for copy in smalls[:2]:
        copy.start()

    fore = obs_dev // stages * 2

    def load(place, part):
        chunk = chunk_at(jnp.int32(place))
        start = pl.multiple_of(chunk * WIDTH, WIDTH)
        at = pl.ds(0, fore) if part == 0 else pl.ds(fore, obs_dev - fore)
        return pltpu.make_async_copy(
            dep.at[pl.ds(start, WIDTH), at],
            window.at[pl.ds(start + HALO, WIDTH), at],
            load_sem.at[part, place],
        )

    strips = [
        pltpu.make_async_copy(dep.at[pl.ds(0, HALO), :], strip.at[0], small_sem.at[6]),
        pltpu.make_async_copy(dep.at[pl.ds(own - HALO, HALO), :], strip.at[1], small_sem.at[7]),
    ]
    for copy in strips + smalls[2:]:
        copy.start()
    for place in range(3):
        load(place, 0).start()

    to_left = pltpu.make_async_remote_copy(
        src_ref=strip.at[0],
        dst_ref=window.at[pl.ds(own + HALO, HALO), :],
        send_sem=halo_send.at[0],
        recv_sem=halo_recv.at[0],
        device_id=peer("chan", left),
        device_id_type=MESH,
    )
    to_right = pltpu.make_async_remote_copy(
        src_ref=strip.at[1],
        dst_ref=window.at[pl.ds(0, HALO), :],
        send_sem=halo_send.at[1],
        recv_sem=halo_recv.at[1],
        device_id=peer("chan", right),
        device_id_type=MESH,
    )

    def meet():
        pl.semaphore_wait(barrier, greeted)
        pl.when(chan > 0)(to_left.start)
        pl.when(chan < n_chan - 1)(to_right.start)

    rim = jnp.zeros((HALO, obs_dev), window.dtype)
    window[own + 2 * HALO :, :] = jnp.zeros((window.shape[0] - own - 2 * HALO, obs_dev), window.dtype)

    @pl.when(chan == 0)
    def _():
        window[:HALO, :] = rim

    @pl.when(chan == n_chan - 1)
    def _():
        window[own + HALO : own + 2 * HALO, :] = rim

    flip[...] = jnp.zeros_like(flip)
    wide[...] = jnp.zeros_like(wide)

    smalls[0].wait()
    smalls[1].wait()
    for place in range(3):
        load(place, 1).start()
    values = pred_in[...].astype(jnp.float32)
    first_row = 0
    for first in range(preds):
        count = preds - first
        wide[first_row : first_row + count, :] = values[first:, :] * values[first : first + 1, :]
        first_row += count
    wide[tall : tall + preds, :] = values

    def mask_line(line, carry):
        at = pl.ds(pl.multiple_of(line * slots, slots), slots)
        slot = lax.broadcasted_iota(jnp.int32, (tall + flat, slots), 1)
        live = jnp.where(slot < counts_in[line], wide[:, at], 0.0).astype(jnp.bfloat16)
        pairs_t[line] = live[:tall, :]
        preds_t[line] = live[tall:, :]
        return carry

    lax.fori_loop(0, lines, mask_line, 0, unroll=4)

    for copy in strips + smalls[2:]:
        copy.wait()
    for part in range(2):
        for place in range(3, 5):
            load(place, part).start()

    @pl.when(chan == 0)
    def _():
        ids_in[:, 0:LANES] = jnp.full((1, LANES), -1, jnp.int32)

    @pl.when(chan == n_chan - 1)
    def _():
        ids_in[:, LANES + own :] = jnp.full((1, LANES), -1, jnp.int32)

    def turn_band(block):
        for part in range(2):
            first = pl.multiple_of(block * WIDTH + part * TILE, TILE)
            own_ids = ids_in[:, pl.ds(first + TILE, TILE)].astype(jnp.float32)
            flip[part, 0:offsets, :] = inv_in[:, pl.ds(first, TILE)].astype(jnp.float32)
            flip[part, 64:65, :] = own_ids
            spun[part] = flip[part].T

    def skew_band(block, side):
        for part in range(2):
            first = pl.multiple_of(block * WIDTH + part * TILE, TILE)
            near = ids_in[:, pl.ds(first, 3 * TILE)].astype(jnp.float32)
            turned = spun[part]
            own_id = turned[:, 64:65]
            place = lax.broadcasted_iota(jnp.int32, turned.shape, 1)
            turned = jnp.where(place < offsets, turned, 0.0)
            skewed = pltpu.roll(
                jnp.concatenate([turned, jnp.zeros_like(turned)], axis=1),
                HALO - half,
                1,
                stride=1,
                stride_axis=0,
            )
            same = near[:, TILE - HALO : 3 * TILE - HALO] == own_id
            band = jnp.where(same, skewed, 0.0).astype(jnp.bfloat16)
            bands[side, part, 0] = band[:, :LANES]
            bands[side, part, 1] = band[:, LANES:]

    def wide_of(ref, first, second):
        return jnp.concatenate([ref[first, second, 0], ref[first, second, 1]], axis=1)

    def paired(ref, at):
        return jnp.concatenate([ref[at // LANES], ref[at // LANES + 1]], axis=1)

    def send_x(level):
        return pltpu.make_async_remote_copy(
            src_ref=x_code.at[level],
            dst_ref=landed_x.at[level],
            send_sem=x_send.at[level],
            recv_sem=x_recv.at[level],
            device_id=peer("obs", partner),
            device_id_type=MESH,
        )

    def send_z(level):
        return pltpu.make_async_remote_copy(
            src_ref=z_code.at[level],
            dst_ref=landed_z.at[lev],
            send_sem=z_send.at[level],
            recv_sem=z_recv.at[lev],
            device_id=peer("obs", 2 * level + col),
            device_id_type=MESH,
        )

    def from_z(level):
        return pltpu.make_async_remote_copy(
            src_ref=z_code.at[0],
            dst_ref=landed_z.at[level],
            send_sem=z_send.at[0],
            recv_sem=z_recv.at[level],
            device_id=peer("obs", 2 * level + col),
            device_id_type=MESH,
        )

    def send_straight(block):
        return pltpu.make_async_remote_copy(
            src_ref=d_code.at[block],
            dst_ref=landed_d.at[me],
            send_sem=d_send.at[block],
            recv_sem=d_recv.at[me],
            device_id=peer("obs", block),
            device_id_type=MESH,
        )

    def from_straight(source):
        return pltpu.make_async_remote_copy(
            src_ref=d_code.at[0],
            dst_ref=landed_d.at[source],
            send_sem=d_send.at[0],
            recv_sem=d_recv.at[source],
            device_id=peer("obs", source),
            device_id_type=MESH,
        )

    def encode(sums):
        gram = sums[:pad]
        rhs = sums[pad:]

        def grade(part):
            most = jnp.max(jnp.abs(part), axis=0, keepdims=True)
            return jnp.ceil(jnp.log2(jnp.maximum(most, 1e-30)))

        gram_grade = grade(gram)
        rhs_grade = grade(rhs)
        row = lax.broadcasted_iota(jnp.int32, rhs.shape, 0)
        gram = gram * (jnp.exp2(-gram_grade) * CODE)
        rhs = rhs * (jnp.exp2(-rhs_grade) * CODE)
        rhs = jnp.where(row == preds, gram_grade, rhs)
        rhs = jnp.where(row == preds + 1, rhs_grade, rhs)
        return jnp.round(jnp.concatenate([gram, rhs], axis=0)).astype(jnp.int32).astype(jnp.int16)

    def decode(code):
        values = code.astype(jnp.int32).astype(jnp.float32)
        gram_scale = jnp.exp2(values[pad + preds : pad + preds + 1]) * (1.0 / CODE)
        rhs_scale = jnp.exp2(values[pad + preds + 1 : pad + preds + 2]) * (1.0 / CODE)
        return jnp.concatenate([values[:pad] * gram_scale, values[pad:] * rhs_scale], axis=0)

    def accumulated(*accs):
        narrow = [[accs[4 * mxu + 2 * side : 4 * mxu + 2 * side + 2] for side in range(2)] for mxu in range(2)]
        tall_acc = [accs[8 + 2 * mxu : 10 + 2 * mxu] for mxu in range(2)]
        flat_acc = [accs[12 + 2 * mxu : 14 + 2 * mxu] for mxu in range(2)]

        def weigh(block, band, stage):
            start = pl.multiple_of(block * WIDTH, WIDTH)
            for mxu in range(2):
                at = (2 * stage + mxu) * OBS_TILE
                for part in range(2):
                    first = pl.multiple_of(start + part * TILE, TILE)
                    pltpu.matmul_push_rhs(
                        window[pl.ds(first, 2 * TILE), at : at + OBS_TILE],
                        staging_register=part,
                        mxu_index=mxu,
                    )
                    pltpu.matmul_acc_lhs(
                        narrow[mxu][stage % 2][part],
                        wide_of(bands, band, part),
                        load_staged_rhs=part,
                    )

        def turn_over(stage):
            for mxu in range(2):
                for part in range(2):
                    weighted = pltpu.matmul_pop(narrow[mxu][stage % 2][part])
                    turned_w[stage % 4, mxu, part] = weighted.astype(jnp.bfloat16).T

        def gather(side, stage):
            edge = jnp.bfloat16(huber_edge)
            for mxu in range(2):
                at = (2 * stage + mxu) * OBS_TILE
                weighted = wide_of(turned_w, stage % 4, mxu)
                qc_weight = edge / jnp.maximum(jnp.abs(weighted), edge)
                scaled = jnp.clip(weighted, -edge, edge)
                pltpu.matmul_push_rhs(qc_weight, staging_register=0, mxu_index=mxu)
                pltpu.matmul_acc_lhs(
                    tall_acc[mxu][side], paired(pairs_t, at), load_staged_rhs=0
                )
                pltpu.matmul_push_rhs(scaled, staging_register=1, mxu_index=mxu)
                pltpu.matmul_acc_lhs(
                    flat_acc[mxu][side], paired(preds_t, at), load_staged_rhs=1
                )

        def result(side):
            gram = pltpu.matmul_pop(tall_acc[0][side]) + pltpu.matmul_pop(tall_acc[1][side])
            rhs = pltpu.matmul_pop(flat_acc[0][side]) + pltpu.matmul_pop(flat_acc[1][side])
            return jnp.concatenate([gram[:pad], rhs], axis=0)

        def keep(step, sums):
            start = pl.multiple_of(block_at(step) * WIDTH, WIDTH)
            part_out[:, pl.ds(start, WIDTH)] = sums

        def joined(step, sums):
            level = level_at(turn_along(step))
            send_x(level).wait_recv()
            return sums + decode(landed_x[level])

        def pass_along(step, sums):
            level = level_at(turn_along(step))
            z_code[level] = encode(joined(step, sums))
            send_z(level).start()

        def deliver(step, sums):
            block = block_at(step)
            own_block = jnp.logical_and(early, block == col)

            @pl.when(jnp.logical_and(straight(step), own_block))
            def _():
                mine[...] = sums

            @pl.when(jnp.logical_and(straight(step), jnp.logical_not(own_block)))
            def _():
                d_code[block] = encode(sums)
                send_straight(block).start()

            @pl.when(across(step))
            def _():
                level = level_across(step)
                x_code[level] = encode(sums)
                send_x(level).start()

            @pl.when(jnp.logical_not(jnp.logical_or(straight(step), across(step))))
            def _():
                pass_along(step, sums)

        for acc in accs:
            pltpu.matmul_pop(acc)
        turn_band(block_at(0))
        skew_band(block_at(0), 0)
        pl.when(jnp.logical_not(early))(meet)
        for part in range(2):
            for place in range(5, blocks):
                load(place, part).start()
        turned_w[2:] = jnp.zeros((2,) + turned_w.shape[1:], turned_w.dtype)
        for place in range(3):
            load(place, 0).wait()
        def half_step(block, side, half_at):
            for stage in (2 * half_at, 2 * half_at + 1):
                weigh(block, side, stage)
            for stage in (2 * half_at, 2 * half_at + 1):
                if half_at == 0:
                    gather(1 - side, stages - 2 + stage)
                else:
                    gather(side, stage - 2)
            for stage in (2 * half_at, 2 * half_at + 1):
                turn_over(stage)

        def one_turn(turn, carry):
            for side in range(2):
                step = 2 * turn + side
                block = block_at(step)
                following = block_at(jnp.minimum(step + 1, blocks - 1))
                more = step + 1 < blocks
                turn_band(following)
                half_step(block, side, 0)
                sums = result(1 - side)
                due = [(place, 1) for place in range(3)] + [(3, 0), (4, 0)]
                if side == 1:
                    due = [(3, 1), (4, 1)]

                @pl.when(turn == 0)
                def _():
                    for place, part in due:
                        load(place, part).wait()
                    pl.when(lev == 1)(load(5, side).wait)

                if side == 0:

                    @pl.when(turn == 1)
                    def _():
                        for part in range(2):
                            pl.when(lev != 1)(load(5, part).wait)
                            for place in range(6, blocks):
                                load(place, part).wait()

                if side == 1:
                    pl.when(jnp.logical_and(early, turn == 0))(meet)

                @pl.when(step > 0)
                def _():
                    if scatter:
                        deliver(step - 1, sums)
                    else:
                        keep(step - 1, sums)

                @pl.when(jnp.logical_and(more, jnp.logical_and(following == 0, chan > 0)))
                def _():
                    to_right.wait_recv()

                @pl.when(
                    jnp.logical_and(
                        more,
                        jnp.logical_and(following == blocks - 1, chan < n_chan - 1),
                    )
                )
                def _():
                    to_left.wait_recv()

                for half_at in range(1, stages // 2):
                    half_step(block, side, half_at)
                skew_band(following, 1 - side)
            return carry

        lax.fori_loop(0, levels, one_turn, 0)
        for stage in range(stages - 2, stages):
            gather(1, stage)
        sums = result(1)
        pl.when(chan > 0)(to_left.wait_send)
        pl.when(chan < n_chan - 1)(to_right.wait_send)
        if not scatter:
            keep(blocks - 1, sums)
            return

        def finish(sums):
            part_out[...] = sums * (1.0 / float(obs_dev * n_obs))

        @pl.when(early)
        def _():
            deliver(blocks - 1, sums)
            whole = mine[...]
            for away in range(1, n_obs):
                source = lax.rem(me + away, n_obs)
                from_straight(source).wait_recv()
                whole = whole + decode(landed_d[source])
            finish(whole)
            for away in range(1, n_obs):
                send_straight(lax.rem(me + away, n_obs)).wait_send()

        @pl.when(jnp.logical_not(early))
        def _():
            whole = joined(blocks - 1, sums)
            for source in range(2):
                from_straight(source).wait_recv()
                whole = whole + decode(landed_d[source])
            for turn in range(levels - 2):
                level = level_at(turn)
                from_z(level).wait_recv()
                whole = whole + decode(landed_z[level])
            finish(whole)
            for block in range(2):
                send_straight(block).wait_send()
            for turn in range(levels - 2):
                send_z(level_at(turn)).wait_send()
            for level in range(1, levels):
                send_x(level).wait_send()

    pl.run_scoped(accumulated, *acc_list(tall, flat))


def spread(preds, pad, part, gram_out, rhs_out, gram, rhs, sems):
    rhs[...] = part[pad : pad + preds, :]
    rhs_copy = pltpu.make_async_copy(rhs, rhs_out, sems.at[0])
    rhs_copy.start()
    for row, source in enumerate(mirror_rows(preds)):
        gram[row : row + 1, :] = part[source : source + 1, :]
    gram_copy = pltpu.make_async_copy(gram, gram_out, sems.at[1])
    gram_copy.start()
    rhs_copy.wait()
    gram_copy.wait()


def acc_list(tall, flat):
    specs = []
    for rows, copies in ((TILE, 4), (tall, 2), (flat, 2)):
        for mxu in range(2):
            specs += [pltpu.ACC(mxu)((rows, OBS_TILE), jnp.float32)] * copies
    return specs


def on_device(departures, predictors, inv_band, band_id, line_counts):
    own, obs_dev = departures.shape
    preds = predictors.shape[0]
    upper = preds * (preds + 1) // 2
    n_obs = lax.axis_size("obs")
    n_chan = lax.axis_size("chan")
    share = own // n_obs
    blocks = own // WIDTH
    scatter = share == WIDTH and n_obs == 8
    pad = padded(upper, 8)
    tall = padded(upper, 16)
    flat = padded(preds + 2, 16)
    rows = pad + flat
    if scatter:
        out_shape = (pltpu.VMEM((rows, share), jnp.float32),)
    else:
        out_shape = (jax.ShapeDtypeStruct((rows, own), jnp.float32),)
    vmem = pl.BlockSpec(memory_space=pltpu.VMEM)
    hbm = pl.BlockSpec(memory_space=pltpu.HBM)
    levels = blocks // 2
    kept = (levels, rows, WIDTH) if scatter else (1, 8, LANES)
    many = (n_obs,) + kept[1:] if scatter else kept
    dma = pltpu.SemaphoreType.DMA
    outs = pl.pallas_call(
        functools.partial(kernel, n_obs, n_chan, scatter),
        out_shape=out_shape,
        in_specs=[hbm] * 5,
        out_specs=tuple(vmem for _ in out_shape),
        scratch_shapes=[
            pltpu.VMEM((own + 4 * HALO, obs_dev), jnp.bfloat16),
            pltpu.VMEM((2, HALO, obs_dev), jnp.bfloat16),
            pltpu.VMEM(predictors.shape, jnp.bfloat16),
            pltpu.VMEM(inv_band.shape, jnp.bfloat16),
            pltpu.VMEM((1, own + 2 * LANES), jnp.int32),
            pltpu.SMEM(line_counts.shape, jnp.int32),
            pltpu.VMEM((tall + flat, obs_dev), jnp.float32),
            pltpu.VMEM((obs_dev // LANES, tall, LANES), jnp.bfloat16),
            pltpu.VMEM((obs_dev // LANES, flat, LANES), jnp.bfloat16),
            pltpu.VMEM((2, LANES, TILE), jnp.float32),
            pltpu.VMEM((2, TILE, LANES), jnp.float32),
            pltpu.VMEM((2, 2, 2, TILE, LANES), jnp.bfloat16),
            pltpu.VMEM((4, 2, 2, OBS_TILE, LANES), jnp.bfloat16),
            pltpu.VMEM((rows, WIDTH), jnp.float32),
            pltpu.VMEM(kept, jnp.int16),
            pltpu.VMEM(kept, jnp.int16),
            pltpu.VMEM(many, jnp.int16),
            pltpu.VMEM(kept, jnp.int16),
            pltpu.VMEM(kept, jnp.int16),
            pltpu.VMEM(many, jnp.int16),
            dma((8,)),
            dma((2, blocks)),
            dma((2,)),
            dma((2,)),
            dma((levels,)),
            dma((levels,)),
            dma((levels,)),
            dma((levels,)),
            dma((n_obs,)),
            dma((n_obs,)),
        ],
        compiler_params=pltpu.CompilerParams(
            collective_id=0,
            has_side_effects=True,
            vmem_limit_bytes=67043328 - 120 * 1024,
        ),
        name="normal_equations",
    )(departures, predictors, inv_band, band_id[None, :], line_counts)
    if scatter:
        return pl.pallas_call(
            functools.partial(spread, preds, pad),
            out_shape=(
                jax.ShapeDtypeStruct((preds * preds, share), jnp.float32),
                jax.ShapeDtypeStruct((preds, share), jnp.float32),
            ),
            in_specs=[vmem],
            out_specs=(hbm, hbm),
            scratch_shapes=[
                pltpu.VMEM((preds * preds, share), jnp.float32),
                pltpu.VMEM((preds, share), jnp.float32),
                dma((2,)),
            ],
            compiler_params=pltpu.CompilerParams(vmem_limit_bytes=1024 * 1024),
            name="mirror",
        )(outs[0])
    factor = 1.0 / float(obs_dev * n_obs)
    part = lax.psum_scatter(outs[0], "obs", scatter_dimension=1, tiled=True) * factor
    mirror = np.array(mirror_rows(preds))
    return part[mirror], part[pad : pad + preds]


def solution(mesh):
    in_specs = (P("chan", "obs"), P(None, "obs"), P(None, "chan"), P(), P("obs"))
    out_specs = (P(None, ("chan", "obs")), P(None, ("chan", "obs")))
    return jax.shard_map(
        on_device, mesh=mesh, in_specs=in_specs, out_specs=out_specs, check_vma=False
    )
```
